32 devices in a mesh: sta: 8 (over z, core), cell: 4 (over y, x).
Axes of the slice: x: 2, y: 2, z: 4, core: 2. Of those that a mesh axis runs over, the one named last changes fastest.
Arguments:
- station_xyz: float32 [3, 2048], P(None, 'sta'), may hold values from 0 to 1, as said below
- cell_xyz: float32 [3, 131072], P(None, 'cell'), may hold values from -0.6 to 1, as said below
- cell_weight: float32 [131072], P('cell'), may hold values from 0.3 to 3
- data: float32 [2048], P(('sta', 'cell')), may hold values from -6 to 6
- model_start: float32 [131072], P(('cell', 'sta')), may hold values from -6 to 6
Outputs:
- model_next: float32 [131072], P(('cell', 'sta'))
- residual_next: float32 [2048], P(('sta', 'cell'))
- search_next: float32 [131072], P(('cell', 'sta'))
The draws below stay inside these ranges and needn't reach their ends.
Inputs may be any that keep to these rules, and one draw needn't show every extreme that they name: `station_xyz`: rows 0 and 1 lie in [0, 1), row 2 in [0, 0.05]. `cell_xyz`: rows 0 and 1 lie in [0, 1), row 2 in [-0.6, -0.02].
All inputs are finite; a program needn't handle non-finite values.
Results may differ from the reference program's by a relative error of at most 0.0003.
Values sent between devices are 32-bit elements; how exact they have to be, the bound alone decides.
A program may use at most 64 MiB of HBM per device.

```python
import math
import jax
import jax.numpy as jnp
from jax import lax

STATIONS = 2048
CELLS = 131072


def draw_station_xyz(key, part):
    plane = jax.random.uniform(jax.random.fold_in(key, 11), (2, STATIONS), jnp.float32, 0.0, 1.0)
    height = jax.random.uniform(jax.random.fold_in(key, 12), (1, STATIONS), jnp.float32, 0.0, 0.05)
    return jnp.concatenate([plane, height], axis=0)


def draw_cell_xyz(key, part):
    plane = jax.random.uniform(jax.random.fold_in(key, 21), (2, CELLS), jnp.float32, 0.0, 1.0)
    depth = jax.random.uniform(jax.random.fold_in(key, 22), (1, CELLS), jnp.float32, -0.6, -0.02)
    return jnp.concatenate([plane, depth], axis=0)


def steps_of(rng, dims, pieces, least, high):
    gain = 1.0
    for axis_at, parts in pieces:
        steps = jax.random.uniform(jax.random.fold_in(jax.random.fold_in(rng, 6), axis_at), (parts,), jnp.float32, least / len(pieces), high / len(pieces))
        gain = gain * jnp.repeat(jnp.exp(steps), dims[axis_at] // parts).reshape((-1,) + (1,) * (len(dims) - 1 - axis_at))
    return gain


def noise(own_key, shape, spread, most, cuts=(), kind=jnp.bfloat16):
    entries = spread * jax.random.normal(own_key, shape, jnp.float32)
    if cuts:
        entries = entries * steps_of(own_key, shape, cuts, -0.22, 0.18)
    return jnp.clip(entries, -most, most).astype(kind)


def setup_inputs(seed: int = 0) -> dict:
    arg_keys = jax.random.split(jax.random.key(seed), 6)
    return {
        "station_xyz": draw_station_xyz(jax.random.fold_in(arg_keys[5], 71), 0),
        "cell_xyz": draw_cell_xyz(jax.random.fold_in(arg_keys[5], 71), 0),
        "cell_weight": jnp.clip(jnp.exp(math.log(3.0) - 2.3025851 * jax.random.uniform(arg_keys[2], (CELLS,), jnp.float32) ** steps_of(arg_keys[2], (CELLS,), ((0, 4),), -0.2, 0.2)), 0.3, 3.0),
        "data": noise(arg_keys[3], (STATIONS,), 1.0, 6.0, ((0, 32),), jnp.float32),
        "model_start": noise(arg_keys[4], (CELLS,), 1.0, 6.0, ((0, 32),), jnp.float32),
    }


SOFT = 0.0001

def kernel(sta, cel, wgt, scale):
    dx = sta[0][:, None] - cel[0][None, :]
    dy = sta[1][:, None] - cel[1][None, :]
    dz = sta[2][:, None] - cel[2][None, :]
    inv = lax.rsqrt(dx * dx + dy * dy + dz * dz + SOFT)
    return scale * dz * inv * inv * inv * wgt[None, :]

def blocked(cel, wgt):
    width = min(8192, cel.shape[1])
    count = cel.shape[1] // width
    return (jnp.transpose(cel.reshape(3, count, width), (1, 0, 2)), wgt.reshape(count, width), count, width)

def forward(sta, cel, wgt, vec, scale):
    cel_b, wgt_b, count, width = blocked(cel, wgt)
    vec_b = vec.reshape(count, width)

    def step(total, item):
        tile = kernel(sta, item[0], item[1], scale)
        return (total + jnp.dot(tile, item[2], precision=lax.Precision.HIGHEST), None)
    total, _ = lax.scan(step, jnp.zeros((sta.shape[1],), jnp.float32), (cel_b, wgt_b, vec_b))
    return total

def backward(sta, cel, wgt, res, scale):
    cel_b, wgt_b, count, width = blocked(cel, wgt)

    def one(item):
        tile = kernel(sta, item[0], item[1], scale)
        return jnp.dot(res, tile, precision=lax.Precision.HIGHEST)
    return lax.map(one, (cel_b, wgt_b)).reshape(-1)

def reference(station_xyz, cell_xyz, cell_weight, data, model_start):
    scale = 1.0 / math.sqrt(STATIONS * CELLS)
    residual = data - forward(station_xyz, cell_xyz, cell_weight, model_start, scale)
    gradient = backward(station_xyz, cell_xyz, cell_weight, residual, scale)
    gamma = jnp.sum(gradient * gradient)
    image = forward(station_xyz, cell_xyz, cell_weight, gradient, scale)
    delta = jnp.sum(image * image)
    alpha = gamma / delta
    model_next = model_start + alpha * gradient
    residual_next = residual - alpha * image
    gradient_next = backward(station_xyz, cell_xyz, cell_weight, residual_next, scale)
    gamma_next = jnp.sum(gradient_next * gradient_next)
    search_next = gradient_next + gamma_next / gamma * gradient
    return (model_next, residual_next, search_next)
```

```python
import functools
import math

import jax
import jax.numpy as jnp
import numpy as np
from jax import lax
from jax.experimental import pallas as pl
from jax.experimental.pallas import tpu as pltpu
from jax.sharding import PartitionSpec as P

SOFT = float(np.float32(0.0001))


def split(value):
    out = []
    for _ in range(3):
        scale = 2.0 ** (math.floor(math.log2(value)) - 7)
        out.append(math.floor(value / scale) * scale)
        value -= out[-1]
    return out


SOFT_PIECES = split(SOFT)
LANES = 128
FEATURES = 80
MESH = pl.DeviceIdType.MESH
F32 = jnp.float32
BF16 = jnp.bfloat16


def pieces(x):
    row = lax.broadcasted_iota(jnp.int32, x.shape, 0)
    x = x + jnp.where(row < 2, -0.5, 0.275)
    x = jnp.where(row < 3, x, 0.0)
    h = jnp.round(x * 256.0) * (1.0 / 256.0)
    rest = x - h
    m = jnp.round(rest * 65536.0) * (1.0 / 65536.0)
    l = rest - m
    a = h * h
    a1 = jnp.round(a * 256.0) * (1.0 / 256.0)
    b = 2.0 * h * rest + rest * rest
    b1 = jnp.round(b * 131072.0) * (1.0 / 131072.0)
    return row, h, m, l, (a1, a - a1, b1, b - b1)


def pair(first, second):
    return first + pltpu.roll(second, 3, 0)


def eight_rows(x):
    return jnp.concatenate([x, jnp.zeros((8 - x.shape[0], x.shape[1]), F32)], axis=0)


def cell_features(x):
    row, h, m, l, (a1, a2, b1, b2) = pieces(x)
    ones = jnp.ones_like(x)
    zero = jnp.zeros_like(x)
    return jnp.concatenate([pair(h, h), pair(h, m), pair(m, m), pair(l, l), l, pair(a1, a2),
                            pair(b1, b2), ones, ones, zero], axis=0).astype(BF16)


def station_features(x):
    row, h, m, l, (a1, a2, b1, b2) = pieces(x)
    ones = jnp.where(row < 6, 1.0, 0.0)
    soft = jnp.where(row == 6, SOFT_PIECES[0], 0.0) + jnp.where(row == 7, SOFT_PIECES[1], 0.0)
    rest = jnp.where(row == 6, SOFT_PIECES[2], 0.0)
    zero = jnp.zeros_like(x)
    h2, m2, l2 = -2.0 * h, -2.0 * m, -2.0 * l
    return jnp.concatenate([pair(h2, m2), pair(l2, h2), pair(m2, l2), pair(h2, m2), l2, ones,
                            ones, pair(a1, a2) + soft, pair(b1, b2) + rest, zero], axis=0)


def kernel(sizes, st_hbm, cell_hbm, w_hbm, m_hbm, data_ref, model_ref, res_ref, search_ref,
           kmat, rhs, lhs, cell_v, w_v, m_all, st_all, szb, urow, acc, gacc, rb, rrow, qrow, grow,
           out1, out2, rs1, rs2, part1, part2, gather1, gather2, gmsg, gnmsg, gout, gnout, dout, din, drow,
           in_sem, st_send, st_recv, m_sem, ar_send, ar_recv1, ar_recv2, ex_send, ex_recv1, ex_recv2,
           sc_send, sc_recv, r2a, r2b):
    n_sta, n_cell, cells, width, piece, scale = sizes
    nz = n_sta // 2
    chips = nz * n_cell
    tiles = 2 * cells // LANES
    half = cells // LANES
    groups = width // 8
    high = width // LANES
    per_tile = LANES // piece
    my_sta, my_cell = lax.axis_index("sta"), lax.axis_index("cell")
    core = lax.rem(my_sta, 2)
    z = lax.div(my_sta, 2)
    chip = z * n_cell + my_cell
    partner = (z * 2 + 1 - core, my_cell)

    def peer(k):
        flat = lax.rem(chip + k, chips)
        return (lax.div(flat, n_cell) * 2 + core, lax.rem(flat, n_cell))

    def every_peer(act):
        if chips > 16 or chips & (chips - 1) or n_cell & (n_cell - 1):
            def one(k, c):
                act(peer(k))
                return c

            lax.fori_loop(1, chips, one, 0)
        else:
            for k in range(1, chips):
                act((my_sta ^ (k // n_cell * 2), my_cell ^ (k % n_cell)))

    def remote(src, dst, send, recv, device):
        return pltpu.make_async_remote_copy(src_ref=src, dst_ref=dst, send_sem=send, recv_sem=recv,
                                            device_id=device, device_id_type=MESH)

    def drain(ref, sem):
        pltpu.make_async_copy(ref, ref, sem).wait()

    first_cell = pl.multiple_of(z * 2 * cells, 2 * cells)
    first_row = pl.multiple_of(z * tiles, tiles)
    load_cells = pltpu.make_async_copy(cell_hbm.at[:, pl.ds(first_cell, 2 * cells)], cell_v, in_sem.at[0])
    load_stations = pltpu.make_async_copy(st_hbm, st_all.at[z], in_sem.at[1])
    load_weights = pltpu.make_async_copy(w_hbm.at[pl.ds(first_row, tiles)], w_v, in_sem.at[2])
    load_model = pltpu.make_async_copy(m_hbm, m_all.at[core], in_sem.at[3])
    load_cells.start()
    load_stations.start()
    load_weights.start()
    load_model.start()

    barrier = pltpu.get_barrier_semaphore()

    every_peer(lambda device: pl.semaphore_signal(barrier, inc=1, device_id=device, device_id_type=MESH))
    pl.semaphore_signal(barrier, inc=1, device_id=partner, device_id_type=MESH)

    def features(n, c):
        cols = pl.ds(pl.multiple_of(n * 512, 512), 512)
        rhs[:, cols] = cell_features(eight_rows(cell_v[:, cols]))
        return c

    load_cells.wait()
    lax.fori_loop(0, 2 * cells // 512, features, 0)

    def prepare(b):
        x = eight_rows(st_all[b])
        feats = station_features(x)
        for i in range(high):
            cols = slice(i * LANES, (i + 1) * LANES)
            lhs[cols, :] = jnp.transpose(feats[:, cols]).astype(BF16)
            zz = jnp.transpose(jnp.broadcast_to(x[2:3, cols], (LANES, LANES)))
            szb[i * 16:(i + 1) * 16] = zz.reshape(16, 8, LANES)

    block = 512
    per_block = block // LANES

    def distances(n, r2):
        cols = pl.ds(pl.multiple_of(n * block, block), block)
        r2[...] = jnp.dot(lhs[...], rhs[:, cols], preferred_element_type=F32).reshape(groups, 8, block)

    def values(b, n, r2):
        at = n * block
        czs = []
        cols = []
        for t in range(per_block):
            cols.append(pl.ds(pl.multiple_of(at + t * LANES, LANES), LANES))
            czs.append(jnp.broadcast_to(cell_v[2:3, cols[t]], (8, LANES)))
        for g in range(groups):
            sz = szb[g]
            for t in range(per_block):
                inv = lax.rsqrt(r2[g, :, t * LANES:(t + 1) * LANES])
                kmat[b * groups + g, :, cols[t]] = ((sz - czs[t]) * inv) * (inv * inv)

    def build(b):
        count = 2 * cells // block
        distances(0, r2a)

        def one(i, c):
            distances(i * 2 + 1, r2b)
            values(b, i * 2, r2a)
            distances(lax.rem(i * 2 + 2, count), r2a)
            values(b, i * 2 + 1, r2b)
            return c

        lax.fori_loop(0, count // 2, one, 0)

    step = 4

    def forward(b, h, add):
        us = [jnp.broadcast_to(urow[pl.ds(h * half + t, 1), :], (8, LANES)) for t in range(half)]

        def some(i, c):
            for j in range(step):
                g = i * step + j
                sums = [None] * 4
                for t in range(half):
                    cols = pl.ds(pl.multiple_of(h * cells + t * LANES, LANES), LANES)
                    value = kmat[b * groups + g, :, cols] * us[t]
                    sums[t % 4] = value if sums[t % 4] is None else sums[t % 4] + value
                value = (sums[0] + sums[1]) + (sums[2] + sums[3])
                acc[b * groups + g] = value + acc[b * groups + g] if add else value
            return c

        lax.fori_loop(0, groups // step, some, 0)

    def block_rows(b):
        rows = []
        for i in range(high):
            x = acc[pl.ds(b * groups + i * 16, 16)].reshape(LANES, LANES)
            rows.append(jnp.sum(jnp.transpose(x), axis=0, keepdims=True))
        return jnp.concatenate(rows, axis=0)

    def send_rows(rows, out, rs, recv, b, which=0):
        out[b] = rows
        rs[b, chip] = rows

        every_peer(lambda device: remote(out.at[b], rs.at[b, chip], ar_send.at[which], recv.at[b],
                                         device).start())

    def broadcast(value, out, msgs, which):
        out[...] = value
        msgs[chip] = value

        every_peer(lambda device: remote(out, msgs.at[chip], sc_send.at[which], sc_recv.at[which],
                                         device).start())

    def order(k):
        return jnp.where(k <= z, z - k, k)

    def settled(j):
        mid = nz // 2
        return jnp.where(lax.rem(j, 2) == 0, mid - 1 - lax.div(j, 2), mid + lax.div(j, 2))

    load_stations.wait()
    prepare(z)
    build(z)

    pl.semaphore_wait(barrier, chips)

    def send_stations(k, c):
        other = lax.rem(z + k, nz)
        remote(st_all.at[z], st_all.at[z], st_send, st_recv.at[z], (other * 2 + core, my_cell)).start()
        return c

    lax.fori_loop(1, nz, send_stations, 0)
    load_model.wait()
    remote(m_all.at[core], m_all.at[core], m_sem.at[0], m_sem.at[1], partner).start()
    load_weights.wait()
    ws = w_v[...] * scale
    w_v[...] = ws
    drain(m_all.at[0], m_sem.at[1])
    urow[...] = ws * m_all[...].reshape(tiles, LANES)

    data = data_ref[...]
    drow[...] = jnp.zeros((high, LANES), F32)
    lane = lax.broadcasted_iota(jnp.int32, (1, LANES), 1)
    wide = jnp.where(lane < piece, jnp.concatenate([data] * per_tile, axis=1), 0.0)
    for q in range(n_cell):
        tile, at = q // per_tile, q % per_tile
        value = pltpu.roll(wide, at * piece, 1) if at else wide
        drow[tile:tile + 1, :] += jnp.where(my_cell == q, value, 0.0)

    forward(z, 0, False)
    forward(z, 1, True)
    send_rows(block_rows(z) - drow[...], out1, rs1, ar_recv1, z)

    def rest(k, c):
        b = order(k)
        drain(st_all.at[b], st_recv.at[b])
        prepare(b)
        build(b)
        forward(b, 0, False)
        forward(b, 1, True)
        send_rows(block_rows(b), out1, rs1, ar_recv1, b)
        return c

    lax.fori_loop(1, nz, rest, 0)

    def arrive(b, rs, recv, store, sign):
        drain(rs.at[b, pl.ds(0, chips - 1)], recv.at[b])
        row = sign * jnp.sum(rs[b], axis=0)
        store[b] = row
        for i in range(high):
            x = jnp.transpose(jnp.broadcast_to(row[i:i + 1], (LANES, LANES)))
            rb[i * 16:(i + 1) * 16] = x.reshape(16, 8, LANES)

    strip = 8

    def backward(b, at):
        rs_ = [rb[g] for g in range(groups)]
        cols = [pl.ds(pl.multiple_of((at + t) * LANES, LANES), LANES) for t in range(strip)]
        out = []
        for t in range(strip):
            total = gacc[at + t]
            for g in range(groups):
                total = total + kmat[b * groups + g, :, cols[t]] * rs_[g]
            out.append(total)
        return out

    def gradient(rs, recv, store, sign, part, gather, send, ex_recv, complete):
        gacc[...] = jnp.zeros((tiles, 8, LANES), F32)

        def early(j, c):
            b = settled(j)
            arrive(b, rs, recv, store, sign)

            def some(i, c):
                for t, total in enumerate(backward(b, i * strip)):
                    gacc[i * strip + t] = total
                return c

            lax.fori_loop(0, tiles // strip, some, 0)
            return c

        lax.fori_loop(0, nz - 1, early, 0)
        b = settled(nz - 1)
        arrive(b, rs, recv, store, sign)
        complete()
        for h in range(2):
            def some(i, c):
                rows = [jnp.sum(a, axis=0, keepdims=True) for a in backward(b, h * half + i * strip)]
                part[h, pl.ds(pl.multiple_of(i * strip, strip), strip)] = jnp.concatenate(rows, axis=0)
                return c

            lax.fori_loop(0, half // strip, some, 0)
            remote(part.at[h], gather.at[h], send, ex_recv.at[h], partner).start()

    gradient(rs1, ar_recv1, rrow, -1.0, part1, gather1, ex_send.at[0], ex_recv1, lambda: None)
    for h in range(2):
        drain(gather1.at[h], ex_recv1.at[h])
        rows = slice(h * half, (h + 1) * half)
        g = w_v[rows] * (part1[h] + gather1[h])
        grow[rows] = g
        urow[rows] = w_v[rows] * g
        if h == 0:
            forward(0, 0, False)
            forward(1, 0, False)
    g = grow[...]
    broadcast(jnp.sum(g * g, axis=0, keepdims=True), gout, gmsg, 0)

    def image(b, c):
        @pl.when(b >= 2)
        def _():
            forward(b, 0, False)

        forward(b, 1, True)
        send_rows(block_rows(b), out2, rs2, ar_recv2, b, 1)
        return c

    lax.fori_loop(0, nz, image, 0)

    def send_delta():
        q = qrow[...]
        dout[...] = jnp.sum(jnp.sum(q * q, axis=0), axis=0, keepdims=True)
        remote(dout, din, sc_send.at[1], sc_recv.at[1], partner).start()

    gradient(rs2, ar_recv2, qrow, 1.0, part2, gather2, ex_send.at[1], ex_recv2, send_delta)

    def total(msgs, which):
        drain(msgs.at[pl.ds(0, chips - 1)], sc_recv.at[which])
        return jnp.sum(jnp.sum(msgs[...], axis=0), axis=1, keepdims=True)

    gamma = total(gmsg, 0)
    drain(din, sc_recv.at[1])
    alpha = gamma / jnp.sum(dout[...] + din[...], axis=1, keepdims=True)

    own = pl.ds(pl.multiple_of(core * half, half), half)
    model_ref[...] = m_all[core] + alpha * grow[own]
    new = rrow[z] - alpha * qrow[z]
    mine = jnp.zeros((1, LANES), F32)
    for q in range(n_cell):
        tile, at = q // per_tile, q % per_tile
        value = new[tile:tile + 1]
        if at:
            value = pltpu.roll(value, LANES - at * piece, 1)
        mine = jnp.where(my_cell == q, value, mine)
    res_ref[...] = mine[:, :piece]

    square = jnp.zeros((half, LANES), F32)
    for h in range(2):
        drain(gather2.at[h], ex_recv2.at[h])
        rows = slice(h * half, (h + 1) * half)
        g = grow[rows] - alpha * (w_v[rows] * (part2[h] + gather2[h]))
        urow[rows] = g
        square += g * g
    broadcast(jnp.sum(square, axis=0, keepdims=True), gnout, gnmsg, 2)
    beta = total(gnmsg, 2) / gamma
    search_ref[...] = urow[own] + beta * grow[own]

    drain(st_all.at[pl.ds(0, nz - 1)], st_send)
    drain(m_all.at[0], m_sem.at[0])
    drain(rs1.at[:, pl.ds(0, chips - 1)], ar_send.at[0])
    drain(rs2.at[:, pl.ds(0, chips - 1)], ar_send.at[1])
    drain(part1, ex_send.at[0])
    drain(part2, ex_send.at[1])
    drain(gmsg.at[pl.ds(0, chips - 1)], sc_send.at[0])
    drain(din, sc_send.at[1])
    drain(gnmsg.at[pl.ds(0, chips - 1)], sc_send.at[2])


def per_device(station_xyz, cell_xyz, cell_weight, data, model_start):
    n_sta, n_cell = lax.axis_size("sta"), lax.axis_size("cell")
    n = n_sta * n_cell
    width = station_xyz.shape[1]
    cells = model_start.shape[0]
    piece = data.shape[0]
    scale = 1.0 / math.sqrt(width * n_sta * cells * n)
    sizes = (n_sta, n_cell, cells, width, piece, scale)
    nz = n_sta // 2
    chips = nz * n_cell
    tiles, half = 2 * cells // LANES, cells // LANES
    groups, high = width // 8, width // LANES
    hbm = pl.BlockSpec(memory_space=pltpu.HBM)
    vmem = pl.BlockSpec(memory_space=pltpu.VMEM)
    spread = pltpu.VMEM((nz * groups, 8, LANES), F32)
    narrow = pltpu.VMEM((groups, 8, LANES), F32)
    lines = pltpu.VMEM((nz, high, LANES), F32)
    whole = pltpu.VMEM((nz, chips, high, LANES), F32)
    halves = pltpu.VMEM((2, half, LANES), F32)
    packed = pltpu.VMEM((tiles, LANES), F32)
    message = pltpu.VMEM((chips, 1, LANES), F32)
    row = pltpu.VMEM((1, LANES), F32)
    dma = pltpu.SemaphoreType.DMA
    model_next, residual, search = pl.pallas_call(
        functools.partial(kernel, sizes),
        out_shape=(jax.ShapeDtypeStruct((half, LANES), F32), jax.ShapeDtypeStruct((1, piece), F32),
                   jax.ShapeDtypeStruct((half, LANES), F32)),
        in_specs=[hbm, hbm, hbm, hbm, vmem],
        out_specs=(vmem, vmem, vmem),
        scratch_shapes=[
            pltpu.VMEM((nz * groups, 8, 2 * cells), F32),
            pltpu.VMEM((FEATURES, 2 * cells), BF16),
            pltpu.VMEM((width, FEATURES), BF16),
            pltpu.VMEM((3, 2 * cells), F32),
            packed, halves,
            pltpu.VMEM((nz, 3, width), F32),
            narrow, packed, spread,
            pltpu.VMEM((tiles, 8, LANES), F32),
            narrow, lines, lines, packed,
            lines, lines, whole, whole,
            halves, halves, halves, halves,
            message, message, row, row, row, row,
            pltpu.VMEM((high, LANES), F32),
            dma((4,)), dma, dma((nz,)), dma((2,)), dma((2,)), dma((nz,)), dma((nz,)),
            dma((2,)), dma((2,)), dma((2,)), dma((3,)), dma((3,)),
            pltpu.VMEM((groups, 8, 512), F32), pltpu.VMEM((groups, 8, 512), F32),
        ],
        compiler_params=pltpu.CompilerParams(
            collective_id=0, has_side_effects=True, vmem_limit_bytes=60 * 1024 * 1024),
    )(station_xyz, cell_xyz, cell_weight.reshape(-1, LANES), model_start.reshape(-1, LANES),
      data.reshape(1, piece))
    return (model_next.reshape(cells), residual.reshape(piece), search.reshape(cells))


def solution(mesh):
    placed = (P(None, "sta"), P(None, "cell"), P("cell"), P(("sta", "cell")), P(("cell", "sta")))
    return jax.shard_map(
        per_device,
        mesh=mesh,
        in_specs=placed,
        out_specs=(P(("cell", "sta")), P(("sta", "cell")), P(("cell", "sta"))),
        check_vma=False,
    )
```

```python
import functools
import math

import jax
import jax.numpy as jnp
import numpy as np
from jax import lax
from jax.experimental import pallas as pl
from jax.experimental.pallas import tpu as pltpu
from jax.sharding import PartitionSpec as P

SOFT = float(np.float32(0.0001))


def split(value):
    out = []
    for _ in range(3):
        scale = 2.0 ** (math.floor(math.log2(value)) - 7)
        out.append(math.floor(value / scale) * scale)
        value -= out[-1]
    return out


SOFT_PIECES = split(SOFT)
LANES = 128
FEATURES = 80
MESH = pl.DeviceIdType.MESH
F32 = jnp.float32
BF16 = jnp.bfloat16


def pieces(x):
    row = lax.broadcasted_iota(jnp.int32, x.shape, 0)
    x = x + jnp.where(row < 2, -0.5, 0.275)
    x = jnp.where(row < 3, x, 0.0)
    h = jnp.round(x * 256.0) * (1.0 / 256.0)
    rest = x - h
    m = jnp.round(rest * 65536.0) * (1.0 / 65536.0)
    l = rest - m
    a = h * h
    a1 = jnp.round(a * 256.0) * (1.0 / 256.0)
    b = 2.0 * h * rest + rest * rest
    b1 = jnp.round(b * 131072.0) * (1.0 / 131072.0)
    return row, h, m, l, (a1, a - a1, b1, b - b1)


def pair(first, second):
    return first + pltpu.roll(second, 3, 0)


def eight_rows(x):
    return jnp.concatenate([x, jnp.zeros((8 - x.shape[0], x.shape[1]), F32)], axis=0)


def cell_features(x):
    row, h, m, l, (a1, a2, b1, b2) = pieces(x)
    ones = jnp.ones_like(x)
    zero = jnp.zeros_like(x)
    return jnp.concatenate([pair(h, h), pair(h, m), pair(m, m), pair(l, l), l, pair(a1, a2),
                            pair(b1, b2), ones, ones, zero], axis=0).astype(BF16)


def station_features(x):
    row, h, m, l, (a1, a2, b1, b2) = pieces(x)
    ones = jnp.where(row < 6, 1.0, 0.0)
    soft = jnp.where(row == 6, SOFT_PIECES[0], 0.0) + jnp.where(row == 7, SOFT_PIECES[1], 0.0)
    rest = jnp.where(row == 6, SOFT_PIECES[2], 0.0)
    zero = jnp.zeros_like(x)
    h2, m2, l2 = -2.0 * h, -2.0 * m, -2.0 * l
    return jnp.concatenate([pair(h2, m2), pair(l2, h2), pair(m2, l2), pair(h2, m2), l2, ones,
                            ones, pair(a1, a2) + soft, pair(b1, b2) + rest, zero], axis=0)


def kernel(sizes, st_hbm, cell_hbm, w_hbm, m_hbm, data_hbm, model_ref, res_ref, search_ref,
           kmat, rhs, lhs, cell_v, w_v, m_all, st_all, szb, urow, acc, gacc, rb, rrow, qrow, grow,
           out1, out2, rs1, rs2, part1, part2, gather1, gather2, gmsg, gnmsg, gout, gnout, dout, din, drow,
           in_sem, st_send, st_recv, m_sem, ar_send, ar_recv1, ar_recv2, ex_send, ex_recv1, ex_recv2,
           sc_send, sc_recv, data_v):
    n_sta, n_cell, cells, width, piece, scale = sizes
    nz = n_sta // 2
    chips = nz * n_cell
    tiles = 2 * cells // LANES
    half = cells // LANES
    groups = width // 8
    high = width // LANES
    per_tile = LANES // piece
    my_sta, my_cell = lax.axis_index("sta"), lax.axis_index("cell")
    core = lax.rem(my_sta, 2)
    z = lax.div(my_sta, 2)
    chip = z * n_cell + my_cell
    partner = (z * 2 + 1 - core, my_cell)

    def peer(k):
        flat = lax.rem(chip + k, chips)
        return (lax.div(flat, n_cell) * 2 + core, lax.rem(flat, n_cell))

    def every_peer(act):
        if chips > 16 or chips & (chips - 1) or n_cell & (n_cell - 1):
            def one(k, c):
                act(peer(k))
                return c

            lax.fori_loop(1, chips, one, 0)
        else:
            for k in range(1, chips):
                act((my_sta ^ (k // n_cell * 2), my_cell ^ (k % n_cell)))

    def remote(src, dst, send, recv, device):
        return pltpu.make_async_remote_copy(src_ref=src, dst_ref=dst, send_sem=send, recv_sem=recv,
                                            device_id=device, device_id_type=MESH)

    def drain(ref, sem):
        pltpu.make_async_copy(ref, ref, sem).wait()

    first_cell = pl.multiple_of(z * 2 * cells, 2 * cells)
    first_row = pl.multiple_of(z * tiles, tiles)
    load_cells = pltpu.make_async_copy(cell_hbm.at[:, pl.ds(first_cell, 2 * cells)], cell_v, in_sem.at[0])
    load_stations = pltpu.make_async_copy(st_hbm, st_all.at[z], in_sem.at[1])
    load_weights = pltpu.make_async_copy(w_hbm.at[pl.ds(first_row, tiles)], w_v, in_sem.at[2])
    load_model = pltpu.make_async_copy(m_hbm, m_all.at[core], in_sem.at[3])
    load_cells.start()
    load_stations.start()
    load_weights.start()
    load_model.start()
    load_data = pltpu.make_async_copy(data_hbm, data_v, in_sem.at[4])
    load_data.start()

    barrier = pltpu.get_barrier_semaphore()

    every_peer(lambda device: pl.semaphore_signal(barrier, inc=1, device_id=device, device_id_type=MESH))
    pl.semaphore_signal(barrier, inc=1, device_id=partner, device_id_type=MESH)

    def features(n, c):
        cols = pl.ds(pl.multiple_of(n * 512, 512), 512)
        rhs[:, cols] = cell_features(eight_rows(cell_v[:, cols]))
        return c

    load_cells.wait()
    lax.fori_loop(0, 2 * cells // 512, features, 0)

    def prepare(b):
        x = eight_rows(st_all[b])
        feats = station_features(x)
        for i in range(high):
            cols = slice(i * LANES, (i + 1) * LANES)
            lhs[cols, :] = jnp.transpose(feats[:, cols]).astype(BF16)
            zz = jnp.transpose(jnp.broadcast_to(x[2:3, cols], (LANES, LANES)))
            szb[i * 16:(i + 1) * 16] = zz.reshape(16, 8, LANES)

    block = min(2048, 2 * cells)

    def build(b, n):
        at = pl.multiple_of(n * block, block)
        r2 = jnp.dot(lhs[...], rhs[:, pl.ds(at, block)], preferred_element_type=F32)
        r2 = r2.reshape(groups, 8, block)
        cz = cell_v[2:3, pl.ds(at, block)]
        out = []
        for t in range(block // LANES):
            cols = slice(t * LANES, (t + 1) * LANES)
            inv = lax.rsqrt(r2[:, :, cols])
            dz = szb[...] - jnp.broadcast_to(cz[:, cols], (8, LANES))[None]
            out.append((dz * inv) * (inv * inv))
        kmat[pl.ds(b * groups, groups), :, pl.ds(at, block)] = jnp.concatenate(out, axis=2)

    def build_from(b, first):
        def one(n, c):
            build(b, n)
            return c

        lax.fori_loop(first, 2 * cells // block, one, 0)

    step = 8

    def forward(b, h, add):
        us = [jnp.broadcast_to(urow[pl.ds(h * half + t, 1), :], (8, LANES)) for t in range(half)]

        def some(i, c):
            for j in range(step):
                g = i * step + j
                sums = [None] * 4
                for t in range(half):
                    cols = pl.ds(pl.multiple_of(h * cells + t * LANES, LANES), LANES)
                    value = kmat[b * groups + g, :, cols] * us[t]
                    sums[t % 4] = value if sums[t % 4] is None else sums[t % 4] + value
                value = (sums[0] + sums[1]) + (sums[2] + sums[3])
                acc[b * groups + g] = value + acc[b * groups + g] if add else value
            return c

        lax.fori_loop(0, groups // step, some, 0)

    def block_rows(b):
        rows = []
        for i in range(high):
            x = acc[pl.ds(b * groups + i * 16, 16)].reshape(LANES, LANES)
            rows.append(jnp.sum(jnp.transpose(x), axis=0, keepdims=True))
        return jnp.concatenate(rows, axis=0)

    def send_rows(rows, out, rs, recv, b, which=0):
        out[b] = rows
        rs[b, chip] = rows

        every_peer(lambda device: remote(out.at[b], rs.at[b, chip], ar_send.at[which], recv.at[b],
                                         device).start())

    def broadcast(value, out, msgs, which):
        out[...] = value
        msgs[chip] = value

        every_peer(lambda device: remote(out, msgs.at[chip], sc_send.at[which], sc_recv.at[which],
                                         device).start())

    def order(k):
        return jnp.where(k <= z, z - k, k)

    def settled(j):
        mid = nz // 2
        return jnp.where(lax.rem(j, 2) == 0, mid - 1 - lax.div(j, 2), mid + lax.div(j, 2))

    load_stations.wait()
    prepare(z)
    build(z, 0)
    pl.semaphore_wait(barrier, chips)

    def send_stations(k, c):
        other = lax.rem(z + k, nz)
        remote(st_all.at[z], st_all.at[z], st_send, st_recv.at[z], (other * 2 + core, my_cell)).start()
        return c

    lax.fori_loop(1, nz, send_stations, 0)
    load_model.wait()
    remote(m_all.at[core], m_all.at[core], m_sem.at[0], m_sem.at[1], partner).start()
    build_from(z, 1)
    load_weights.wait()
    ws = w_v[...] * scale
    w_v[...] = ws
    drain(m_all.at[0], m_sem.at[1])
    urow[...] = ws * m_all[...].reshape(tiles, LANES)

    load_data.wait()
    data = data_v[...]
    drow[...] = jnp.zeros((high, LANES), F32)
    lane = lax.broadcasted_iota(jnp.int32, (1, LANES), 1)
    wide = jnp.where(lane < piece, jnp.concatenate([data] * per_tile, axis=1), 0.0)
    for q in range(n_cell):
        tile, at = q // per_tile, q % per_tile
        value = pltpu.roll(wide, at * piece, 1) if at else wide
        drow[tile:tile + 1, :] += jnp.where(my_cell == q, value, 0.0)

    forward(z, 0, False)
    forward(z, 1, True)
    send_rows(block_rows(z) - drow[...], out1, rs1, ar_recv1, z)

    def rest(k, c):
        b = order(k)
        drain(st_all.at[b], st_recv.at[b])
        prepare(b)
        build_from(b, 0)
        forward(b, 0, False)
        forward(b, 1, True)
        send_rows(block_rows(b), out1, rs1, ar_recv1, b)
        return c

    lax.fori_loop(1, nz, rest, 0)

    def arrive(b, rs, recv, store, sign):
        drain(rs.at[b, pl.ds(0, chips - 1)], recv.at[b])
        row = sign * jnp.sum(rs[b], axis=0)
        store[b] = row
        for i in range(high):
            x = jnp.transpose(jnp.broadcast_to(row[i:i + 1], (LANES, LANES)))
            rb[i * 16:(i + 1) * 16] = x.reshape(16, 8, LANES)

    strip = 16

    def backward(b, at):
        x = kmat[pl.ds(b * groups, groups), :, pl.ds(pl.multiple_of(at * LANES, LANES), strip * LANES)]
        return [gacc[at + t] + jnp.sum(x[:, :, t * LANES:(t + 1) * LANES] * rb[...], axis=0)
                for t in range(strip)]

    def gradient(rs, recv, store, sign, part, gather, send, ex_recv, complete):
        gacc[...] = jnp.zeros((tiles, 8, LANES), F32)

        def early(j, c):
            b = settled(j)
            arrive(b, rs, recv, store, sign)

            def some(i, c):
                for t, total in enumerate(backward(b, i * strip)):
                    gacc[i * strip + t] = total
                return c

            lax.fori_loop(0, tiles // strip, some, 0)
            return c

        lax.fori_loop(0, nz - 1, early, 0)
        b = settled(nz - 1)
        arrive(b, rs, recv, store, sign)
        complete()
        for h in range(2):
            def some(i, c):
                rows = [jnp.sum(a, axis=0, keepdims=True) for a in backward(b, h * half + i * strip)]
                part[h, pl.ds(pl.multiple_of(i * strip, strip), strip)] = jnp.concatenate(rows, axis=0)
                return c

            lax.fori_loop(0, half // strip, some, 0)
            remote(part.at[h], gather.at[h], send, ex_recv.at[h], partner).start()

    gradient(rs1, ar_recv1, rrow, -1.0, part1, gather1, ex_send.at[0], ex_recv1, lambda: None)
    for h in range(2):
        drain(gather1.at[h], ex_recv1.at[h])
        rows = slice(h * half, (h + 1) * half)
        g = w_v[rows] * (part1[h] + gather1[h])
        grow[rows] = g
        urow[rows] = w_v[rows] * g
        if h == 0:
            forward(settled(0), 0, False)
            forward(settled(1), 0, False)
    g = grow[...]
    broadcast(jnp.sum(g * g, axis=0, keepdims=True), gout, gmsg, 0)

    def image(j, c):
        b = settled(j)

        @pl.when(j >= 2)
        def _():
            forward(b, 0, False)

        forward(b, 1, True)
        send_rows(block_rows(b), out2, rs2, ar_recv2, b, 1)
        return c

    lax.fori_loop(0, nz, image, 0)

    def send_delta():
        q = qrow[...]
        dout[...] = jnp.sum(jnp.sum(q * q, axis=0), axis=0, keepdims=True)
        remote(dout, din, sc_send.at[1], sc_recv.at[1], partner).start()

    gradient(rs2, ar_recv2, qrow, 1.0, part2, gather2, ex_send.at[1], ex_recv2, send_delta)

    def total(msgs, which):
        drain(msgs.at[pl.ds(0, chips - 1)], sc_recv.at[which])
        return jnp.sum(jnp.sum(msgs[...], axis=0), axis=1, keepdims=True)

    gamma = total(gmsg, 0)
    drain(din, sc_recv.at[1])
    alpha = gamma / jnp.sum(dout[...] + din[...], axis=1, keepdims=True)

    own = pl.ds(pl.multiple_of(core * half, half), half)
    model_ref[...] = m_all[core] + alpha * grow[own]
    new = rrow[z] - alpha * qrow[z]
    mine = jnp.zeros((1, LANES), F32)
    for q in range(n_cell):
        tile, at = q // per_tile, q % per_tile
        value = new[tile:tile + 1]
        if at:
            value = pltpu.roll(value, LANES - at * piece, 1)
        mine = jnp.where(my_cell == q, value, mine)
    res_ref[...] = mine[:, :piece]

    square = jnp.zeros((half, LANES), F32)
    for h in range(2):
        drain(gather2.at[h], ex_recv2.at[h])
        rows = slice(h * half, (h + 1) * half)
        g = grow[rows] - alpha * (w_v[rows] * (part2[h] + gather2[h]))
        urow[rows] = g
        square += g * g
    broadcast(jnp.sum(square, axis=0, keepdims=True), gnout, gnmsg, 2)
    beta = total(gnmsg, 2) / gamma
    search_ref[...] = urow[own] + beta * grow[own]

    drain(st_all.at[pl.ds(0, nz - 1)], st_send)
    drain(m_all.at[0], m_sem.at[0])
    drain(rs1.at[:, pl.ds(0, chips - 1)], ar_send.at[0])
    drain(rs2.at[:, pl.ds(0, chips - 1)], ar_send.at[1])
    drain(part1, ex_send.at[0])
    drain(part2, ex_send.at[1])
    drain(gmsg.at[pl.ds(0, chips - 1)], sc_send.at[0])
    drain(din, sc_send.at[1])
    drain(gnmsg.at[pl.ds(0, chips - 1)], sc_send.at[2])


def per_device(station_xyz, cell_xyz, cell_weight, data, model_start):
    n_sta, n_cell = lax.axis_size("sta"), lax.axis_size("cell")
    n = n_sta * n_cell
    width = station_xyz.shape[1]
    cells = model_start.shape[0]
    piece = data.shape[0]
    scale = 1.0 / math.sqrt(width * n_sta * cells * n)
    sizes = (n_sta, n_cell, cells, width, piece, scale)
    nz = n_sta // 2
    chips = nz * n_cell
    tiles, half = 2 * cells // LANES, cells // LANES
    groups, high = width // 8, width // LANES
    hbm = pl.BlockSpec(memory_space=pltpu.HBM)
    vmem = pl.BlockSpec(memory_space=pltpu.VMEM)
    spread = pltpu.VMEM((nz * groups, 8, LANES), F32)
    narrow = pltpu.VMEM((groups, 8, LANES), F32)
    lines = pltpu.VMEM((nz, high, LANES), F32)
    whole = pltpu.VMEM((nz, chips, high, LANES), F32)
    halves = pltpu.VMEM((2, half, LANES), F32)
    packed = pltpu.VMEM((tiles, LANES), F32)
    message = pltpu.VMEM((chips, 1, LANES), F32)
    row = pltpu.VMEM((1, LANES), F32)
    dma = pltpu.SemaphoreType.DMA
    model_next, residual, search = pl.pallas_call(
        functools.partial(kernel, sizes),
        out_shape=(jax.ShapeDtypeStruct((half, LANES), F32), jax.ShapeDtypeStruct((1, piece), F32),
                   jax.ShapeDtypeStruct((half, LANES), F32)),
        in_specs=[hbm] * 5,
        out_specs=(vmem, vmem, vmem),
        scratch_shapes=[
            pltpu.VMEM((nz * groups, 8, 2 * cells), F32),
            pltpu.VMEM((FEATURES, 2 * cells), BF16),
            pltpu.VMEM((width, FEATURES), BF16),
            pltpu.VMEM((3, 2 * cells), F32),
            packed, halves,
            pltpu.VMEM((nz, 3, width), F32),
            narrow, packed, spread,
            pltpu.VMEM((tiles, 8, LANES), F32),
            narrow, lines, lines, packed,
            lines, lines, whole, whole,
            halves, halves, halves, halves,
            message, message, row, row, row, row,
            pltpu.VMEM((high, LANES), F32),
            dma((5,)), dma, dma((nz,)), dma((2,)), dma((2,)), dma((nz,)), dma((nz,)),
            dma((2,)), dma((2,)), dma((2,)), dma((3,)), dma((3,)),
            pltpu.VMEM((1, piece), F32),
        ],
        compiler_params=pltpu.CompilerParams(
            collective_id=0, has_side_effects=True, vmem_limit_bytes=60 * 1024 * 1024),
    )(station_xyz, cell_xyz, cell_weight.reshape(-1, LANES), model_start.reshape(-1, LANES),
      data.reshape(1, piece))
    return (model_next.reshape(cells), residual.reshape(piece), search.reshape(cells))


def solution(mesh):
    placed = (P(None, "sta"), P(None, "cell"), P("cell"), P(("sta", "cell")), P(("cell", "sta")))
    return jax.shard_map(
        per_device,
        mesh=mesh,
        in_specs=placed,
        out_specs=(P(("cell", "sta")), P(("sta", "cell")), P(("cell", "sta"))),
        check_vma=False,
    )
```

```python
import functools
import math

import jax
import jax.numpy as jnp
import numpy as np
from jax import lax
from jax.experimental import pallas as pl
from jax.experimental.pallas import tpu as pltpu
from jax.sharding import PartitionSpec as P

SOFT = float(np.float32(0.0001))


def split(value):
    out = []
    for _ in range(3):
        scale = 2.0 ** (math.floor(math.log2(value)) - 7)
        out.append(math.floor(value / scale) * scale)
        value -= out[-1]
    return out


SOFT_PIECES = split(SOFT)
LANES = 128
FEATURES = 80
MESH = pl.DeviceIdType.MESH
F32 = jnp.float32
BF16 = jnp.bfloat16


def pieces(x):
    row = lax.broadcasted_iota(jnp.int32, x.shape, 0)
    x = x + jnp.where(row < 2, -0.5, 0.275)
    x = jnp.where(row < 3, x, 0.0)
    h = jnp.round(x * 256.0) * (1.0 / 256.0)
    rest = x - h
    m = jnp.round(rest * 65536.0) * (1.0 / 65536.0)
    l = rest - m
    a = h * h
    a1 = jnp.round(a * 256.0) * (1.0 / 256.0)
    b = 2.0 * h * rest + rest * rest
    b1 = jnp.round(b * 131072.0) * (1.0 / 131072.0)
    return row, h, m, l, (a1, a - a1, b1, b - b1)


def pair(first, second):
    return first + pltpu.roll(second, 3, 0)


def eight_rows(x):
    return jnp.concatenate([x, jnp.zeros((8 - x.shape[0], x.shape[1]), F32)], axis=0)


def cell_features(x):
    row, h, m, l, (a1, a2, b1, b2) = pieces(x)
    ones = jnp.ones_like(x)
    zero = jnp.zeros_like(x)
    return jnp.concatenate([pair(h, h), pair(h, m), pair(m, m), pair(l, l), l, pair(a1, a2),
                            pair(b1, b2), ones, ones, zero], axis=0).astype(BF16)


def station_features(x):
    row, h, m, l, (a1, a2, b1, b2) = pieces(x)
    ones = jnp.where(row < 6, 1.0, 0.0)
    soft = jnp.where(row == 6, SOFT_PIECES[0], 0.0) + jnp.where(row == 7, SOFT_PIECES[1], 0.0)
    rest = jnp.where(row == 6, SOFT_PIECES[2], 0.0)
    zero = jnp.zeros_like(x)
    h2, m2, l2 = -2.0 * h, -2.0 * m, -2.0 * l
    return jnp.concatenate([pair(h2, m2), pair(l2, h2), pair(m2, l2), pair(h2, m2), l2, ones,
                            ones, pair(a1, a2) + soft, pair(b1, b2) + rest, zero], axis=0)


def kernel(sizes, st_hbm, cell_hbm, w_hbm, m_hbm, data_hbm, model_ref, res_ref, search_ref,
           kmat, rhs, lhs, cell_v, w_v, m_all, st_all, szb, urow, acc, gacc, rb, rrow, qrow, grow,
           out1, out2, rs1, rs2, part1, part2, gather1, gather2, gmsg, gnmsg, gout, gnout, dout, din, drow,
           in_sem, st_send, st_recv, m_sem, ar_send, ar_recv1, ar_recv2, ex_send, ex_recv1, ex_recv2,
           sc_send, sc_recv, data_v):
    n_sta, n_cell, cells, width, piece, scale = sizes
    nz = n_sta // 2
    chips = nz * n_cell
    tiles = 2 * cells // LANES
    half = cells // LANES
    groups = width // 8
    high = width // LANES
    per_tile = LANES // piece
    my_sta, my_cell = lax.axis_index("sta"), lax.axis_index("cell")
    core = lax.rem(my_sta, 2)
    z = lax.div(my_sta, 2)
    chip = z * n_cell + my_cell
    partner = (z * 2 + 1 - core, my_cell)

    def peer(k):
        flat = lax.rem(chip + k, chips)
        return (lax.div(flat, n_cell) * 2 + core, lax.rem(flat, n_cell))

    def every_peer(act):
        if chips > 16 or chips & (chips - 1) or n_cell & (n_cell - 1):
            def one(k, c):
                act(peer(k))
                return c

            lax.fori_loop(1, chips, one, 0)
        else:
            for k in range(chips - 1, 0, -1):
                act((my_sta ^ (k // n_cell * 2), my_cell ^ (k % n_cell)))

    def remote(src, dst, send, recv, device):
        return pltpu.make_async_remote_copy(src_ref=src, dst_ref=dst, send_sem=send, recv_sem=recv,
                                            device_id=device, device_id_type=MESH)

    def drain(ref, sem):
        pltpu.make_async_copy(ref, ref, sem).wait()

    barrier = pltpu.get_barrier_semaphore()

    every_peer(lambda device: pl.semaphore_signal(barrier, inc=1, device_id=device, device_id_type=MESH))
    pl.semaphore_signal(barrier, inc=1, device_id=partner, device_id_type=MESH)

    first_cell = pl.multiple_of(z * 2 * cells, 2 * cells)
    first_row = pl.multiple_of(z * tiles, tiles)
    load_cells = pltpu.make_async_copy(cell_hbm.at[:, pl.ds(first_cell, 2 * cells)], cell_v, in_sem.at[0])
    load_stations = pltpu.make_async_copy(st_hbm, st_all.at[z], in_sem.at[1])
    load_weights = pltpu.make_async_copy(w_hbm.at[pl.ds(first_row, tiles)], w_v, in_sem.at[2])
    load_model = pltpu.make_async_copy(m_hbm, m_all.at[core], in_sem.at[3])
    load_cells.start()
    load_stations.start()
    load_weights.start()
    load_model.start()
    load_data = pltpu.make_async_copy(data_hbm, data_v, in_sem.at[4])
    load_data.start()

    def features(n, c):
        cols = pl.ds(pl.multiple_of(n * 512, 512), 512)
        rhs[:, cols] = cell_features(eight_rows(cell_v[:, cols]))
        return c

    load_cells.wait()
    lax.fori_loop(0, 2 * cells // 512, features, 0)

    def prepare(b):
        x = eight_rows(st_all[b])
        feats = station_features(x)
        for i in range(high):
            cols = slice(i * LANES, (i + 1) * LANES)
            lhs[cols, :] = jnp.transpose(feats[:, cols]).astype(BF16)
            zz = jnp.transpose(jnp.broadcast_to(x[2:3, cols], (LANES, LANES)))
            szb[i * 16:(i + 1) * 16] = zz.reshape(16, 8, LANES)

    block = min(2048, 2 * cells)

    def build(b, n):
        at = pl.multiple_of(n * block, block)
        r2 = jnp.dot(lhs[...], rhs[:, pl.ds(at, block)], preferred_element_type=F32)
        r2 = r2.reshape(groups, 8, block)
        cz = cell_v[2:3, pl.ds(at, block)]
        out = []
        for t in range(block // LANES):
            cols = slice(t * LANES, (t + 1) * LANES)
            inv = lax.rsqrt(r2[:, :, cols])
            dz = szb[...] - jnp.broadcast_to(cz[:, cols], (8, LANES))[None]
            out.append((dz * inv) * (inv * inv))
        kmat[pl.ds(b * groups, groups), :, pl.ds(at, block)] = jnp.concatenate(out, axis=2)

    def build_from(b, first):
        def one(n, c):
            build(b, n)
            return c

        lax.fori_loop(first, 2 * cells // block, one, 0)

    step = 8

    def forward(b, h, add):
        us = [jnp.broadcast_to(urow[pl.ds(h * half + t, 1), :], (8, LANES)) for t in range(half)]

        def some(i, c):
            for j in range(step):
                g = i * step + j
                sums = [None] * 4
                for t in range(half):
                    cols = pl.ds(pl.multiple_of(h * cells + t * LANES, LANES), LANES)
                    value = kmat[b * groups + g, :, cols] * us[t]
                    sums[t % 4] = value if sums[t % 4] is None else sums[t % 4] + value
                value = (sums[0] + sums[1]) + (sums[2] + sums[3])
                acc[b * groups + g] = value + acc[b * groups + g] if add else value
            return c

        lax.fori_loop(0, groups // step, some, 0)

    def block_rows(b):
        rows = []
        for i in range(high):
            x = acc[pl.ds(b * groups + i * 16, 16)].reshape(LANES, LANES)
            rows.append(jnp.sum(jnp.transpose(x), axis=0, keepdims=True))
        return jnp.concatenate(rows, axis=0)

    def send_rows(rows, out, rs, recv, b, which=0):
        out[b] = rows
        rs[b, chip] = rows

        every_peer(lambda device: remote(out.at[b], rs.at[b, chip], ar_send.at[which], recv.at[b],
                                         device).start())

    def broadcast(value, out, msgs, which):
        out[...] = value
        msgs[chip] = value

        every_peer(lambda device: remote(out, msgs.at[chip], sc_send.at[which], sc_recv.at[which],
                                         device).start())

    def order(k):
        return jnp.where(k <= z, z - k, k)

    def settled(j):
        mid = nz // 2
        return jnp.where(lax.rem(j, 2) == 0, mid - 1 - lax.div(j, 2), mid + lax.div(j, 2))

    load_stations.wait()
    prepare(z)
    build(z, 0)
    pl.semaphore_wait(barrier, chips)

    def send_stations(k, c):
        other = lax.rem(z + k, nz)
        remote(st_all.at[z], st_all.at[z], st_send, st_recv.at[z], (other * 2 + core, my_cell)).start()
        return c

    lax.fori_loop(1, nz, send_stations, 0)
    load_model.wait()
    remote(m_all.at[core], m_all.at[core], m_sem.at[0], m_sem.at[1], partner).start()
    build_from(z, 1)
    load_weights.wait()
    ws = w_v[...] * scale
    w_v[...] = ws
    drain(m_all.at[0], m_sem.at[1])
    urow[...] = ws * m_all[...].reshape(tiles, LANES)

    load_data.wait()
    data = data_v[...]
    drow[...] = jnp.zeros((high, LANES), F32)
    lane = lax.broadcasted_iota(jnp.int32, (1, LANES), 1)
    wide = jnp.where(lane < piece, jnp.concatenate([data] * per_tile, axis=1), 0.0)
    for q in range(n_cell):
        tile, at = q // per_tile, q % per_tile
        value = pltpu.roll(wide, at * piece, 1) if at else wide
        drow[tile:tile + 1, :] += jnp.where(my_cell == q, value, 0.0)

    forward(z, 0, False)
    forward(z, 1, True)

    def rest(k, c):
        b = order(k)
        drain(st_all.at[b], st_recv.at[b])
        rows = block_rows(order(k - 1)) - jnp.where(k == 1, drow[...], 0.0)
        prepare(b)
        send_rows(rows, out1, rs1, ar_recv1, order(k - 1))
        build_from(b, 0)
        forward(b, 0, False)
        forward(b, 1, True)
        return c

    lax.fori_loop(1, nz, rest, 0)
    send_rows(block_rows(order(nz - 1)), out1, rs1, ar_recv1, order(nz - 1))

    def arrive(b, rs, recv, store, sign):
        drain(rs.at[b, pl.ds(0, chips - 1)], recv.at[b])
        row = sign * jnp.sum(rs[b], axis=0)
        store[b] = row
        for i in range(high):
            x = jnp.transpose(jnp.broadcast_to(row[i:i + 1], (LANES, LANES)))
            rb[i * 16:(i + 1) * 16] = x.reshape(16, 8, LANES)

    strip = 16

    def backward(b, at):
        x = kmat[pl.ds(b * groups, groups), :, pl.ds(pl.multiple_of(at * LANES, LANES), strip * LANES)]
        return [gacc[at + t] + jnp.sum(x[:, :, t * LANES:(t + 1) * LANES] * rb[...], axis=0)
                for t in range(strip)]

    def gradient(rs, recv, store, sign, part, gather, send, ex_recv, complete):
        gacc[...] = jnp.zeros((tiles, 8, LANES), F32)

        def early(j, c):
            b = settled(j)
            arrive(b, rs, recv, store, sign)

            def some(i, c):
                for t, total in enumerate(backward(b, i * strip)):
                    gacc[i * strip + t] = total
                return c

            lax.fori_loop(0, tiles // strip, some, 0)
            return c

        lax.fori_loop(0, nz - 1, early, 0)
        b = settled(nz - 1)
        arrive(b, rs, recv, store, sign)
        complete()
        for h in range(2):
            def some(i, c):
                rows = [jnp.sum(a, axis=0, keepdims=True) for a in backward(b, h * half + i * strip)]
                part[h, pl.ds(pl.multiple_of(i * strip, strip), strip)] = jnp.concatenate(rows, axis=0)
                return c

            lax.fori_loop(0, half // strip, some, 0)
            remote(part.at[h], gather.at[h], send, ex_recv.at[h], partner).start()

    gradient(rs1, ar_recv1, rrow, -1.0, part1, gather1, ex_send.at[0], ex_recv1, lambda: None)
    for h in range(2):
        drain(gather1.at[h], ex_recv1.at[h])
        rows = slice(h * half, (h + 1) * half)
        g = w_v[rows] * (part1[h] + gather1[h])
        grow[rows] = g
        urow[rows] = w_v[rows] * g
        if h == 0:
            forward(settled(0), 0, False)
            forward(settled(1), 0, False)
    g = grow[...]
    broadcast(jnp.sum(g * g, axis=0, keepdims=True), gout, gmsg, 0)

    def image(j, c):
        b = settled(j)

        @pl.when(j >= 2)
        def _():
            forward(b, 0, False)

        forward(b, 1, True)
        send_rows(block_rows(b), out2, rs2, ar_recv2, b, 1)
        return c

    lax.fori_loop(0, nz, image, 0)

    def send_delta():
        q = qrow[...]
        dout[...] = jnp.sum(jnp.sum(q * q, axis=0), axis=0, keepdims=True)
        remote(dout, din, sc_send.at[1], sc_recv.at[1], partner).start()

    gradient(rs2, ar_recv2, qrow, 1.0, part2, gather2, ex_send.at[1], ex_recv2, send_delta)

    def total(msgs, which):
        drain(msgs.at[pl.ds(0, chips - 1)], sc_recv.at[which])
        return jnp.sum(jnp.sum(msgs[...], axis=0), axis=1, keepdims=True)

    gamma = total(gmsg, 0)
    drain(din, sc_recv.at[1])
    alpha = gamma / jnp.sum(dout[...] + din[...], axis=1, keepdims=True)

    own = pl.ds(pl.multiple_of(core * half, half), half)
    model_ref[...] = m_all[core] + alpha * grow[own]
    new = rrow[z] - alpha * qrow[z]
    mine = jnp.zeros((1, LANES), F32)
    for q in range(n_cell):
        tile, at = q // per_tile, q % per_tile
        value = new[tile:tile + 1]
        if at:
            value = pltpu.roll(value, LANES - at * piece, 1)
        mine = jnp.where(my_cell == q, value, mine)
    res_ref[...] = mine[:, :piece]

    square = jnp.zeros((half, LANES), F32)
    for h in range(2):
        drain(gather2.at[h], ex_recv2.at[h])
        rows = slice(h * half, (h + 1) * half)
        g = grow[rows] - alpha * (w_v[rows] * (part2[h] + gather2[h]))
        urow[rows] = g
        square += g * g
    broadcast(jnp.sum(square, axis=0, keepdims=True), gnout, gnmsg, 2)
    beta = total(gnmsg, 2) / gamma
    search_ref[...] = urow[own] + beta * grow[own]

    drain(st_all.at[pl.ds(0, nz - 1)], st_send)
    drain(m_all.at[0], m_sem.at[0])
    drain(rs1.at[:, pl.ds(0, chips - 1)], ar_send.at[0])
    drain(rs2.at[:, pl.ds(0, chips - 1)], ar_send.at[1])
    drain(part1, ex_send.at[0])
    drain(part2, ex_send.at[1])
    drain(gmsg.at[pl.ds(0, chips - 1)], sc_send.at[0])
    drain(din, sc_send.at[1])
    drain(gnmsg.at[pl.ds(0, chips - 1)], sc_send.at[2])


def per_device(station_xyz, cell_xyz, cell_weight, data, model_start):
    n_sta, n_cell = lax.axis_size("sta"), lax.axis_size("cell")
    n = n_sta * n_cell
    width = station_xyz.shape[1]
    cells = model_start.shape[0]
    piece = data.shape[0]
    scale = 1.0 / math.sqrt(width * n_sta * cells * n)
    sizes = (n_sta, n_cell, cells, width, piece, scale)
    nz = n_sta // 2
    chips = nz * n_cell
    tiles, half = 2 * cells // LANES, cells // LANES
    groups, high = width // 8, width // LANES
    hbm = pl.BlockSpec(memory_space=pltpu.HBM)
    vmem = pl.BlockSpec(memory_space=pltpu.VMEM)
    spread = pltpu.VMEM((nz * groups, 8, LANES), F32)
    narrow = pltpu.VMEM((groups, 8, LANES), F32)
    lines = pltpu.VMEM((nz, high, LANES), F32)
    whole = pltpu.VMEM((nz, chips, high, LANES), F32)
    halves = pltpu.VMEM((2, half, LANES), F32)
    packed = pltpu.VMEM((tiles, LANES), F32)
    message = pltpu.VMEM((chips, 1, LANES), F32)
    row = pltpu.VMEM((1, LANES), F32)
    dma = pltpu.SemaphoreType.DMA
    model_next, residual, search = pl.pallas_call(
        functools.partial(kernel, sizes),
        out_shape=(jax.ShapeDtypeStruct((half, LANES), F32), jax.ShapeDtypeStruct((1, piece), F32),
                   jax.ShapeDtypeStruct((half, LANES), F32)),
        in_specs=[hbm] * 5,
        out_specs=(vmem, vmem, vmem),
        scratch_shapes=[
            pltpu.VMEM((nz * groups, 8, 2 * cells), F32),
            pltpu.VMEM((FEATURES, 2 * cells), BF16),
            pltpu.VMEM((width, FEATURES), BF16),
            pltpu.VMEM((3, 2 * cells), F32),
            packed, halves,
            pltpu.VMEM((nz, 3, width), F32),
            narrow, packed, spread,
            pltpu.VMEM((tiles, 8, LANES), F32),
            narrow, lines, lines, packed,
            lines, lines, whole, whole,
            halves, halves, halves, halves,
            message, message, row, row, row, row,
            pltpu.VMEM((high, LANES), F32),
            dma((5,)), dma, dma((nz,)), dma((2,)), dma((2,)), dma((nz,)), dma((nz,)),
            dma((2,)), dma((2,)), dma((2,)), dma((3,)), dma((3,)),
            pltpu.VMEM((1, piece), F32),
        ],
        compiler_params=pltpu.CompilerParams(
            collective_id=0, has_side_effects=True, vmem_limit_bytes=48 * 1024 * 1024),
    )(*[pltpu.with_memory_space_constraint(x, pltpu.HBM) for x in (station_xyz, cell_xyz, cell_weight.reshape(-1, LANES), model_start.reshape(-1, LANES),
      data.reshape(1, piece))])
    def hand(a, b, c, x, y, z):
        x[...] = a[...]
        y[...] = b[...]
        z[...] = c[...]

    model_next, residual, search = pl.pallas_call(
        hand,
        out_shape=(jax.ShapeDtypeStruct((half, LANES), F32), jax.ShapeDtypeStruct((1, piece), F32),
                   jax.ShapeDtypeStruct((half, LANES), F32)),
        in_specs=[vmem] * 3, out_specs=(vmem, vmem, vmem),
        compiler_params=pltpu.CompilerParams(vmem_limit_bytes=1024 * 1024),
    )(model_next, residual, search)
    return (model_next.reshape(cells), residual.reshape(piece), search.reshape(cells))


def solution(mesh):
    placed = (P(None, "sta"), P(None, "cell"), P("cell"), P(("sta", "cell")), P(("cell", "sta")))
    return jax.shard_map(
        per_device,
        mesh=mesh,
        in_specs=placed,
        out_specs=(P(("cell", "sta")), P(("sta", "cell")), P(("cell", "sta"))),
        check_vma=False,
    )
```

```python
import functools
import math

import jax
import jax.numpy as jnp
import numpy as np
from jax import lax
from jax.experimental import pallas as pl
from jax.experimental.pallas import tpu as pltpu
from jax.sharding import PartitionSpec as P

SOFT = float(np.float32(0.0001))


def split(value):
    out = []
    for _ in range(3):
        scale = 2.0 ** (math.floor(math.log2(value)) - 7)
        out.append(math.floor(value / scale) * scale)
        value -= out[-1]
    return out


SOFT_PIECES = split(SOFT)
LANES = 128
FEATURES = 80
MESH = pl.DeviceIdType.MESH
F32 = jnp.float32
BF16 = jnp.bfloat16


def pieces(x):
    row = lax.broadcasted_iota(jnp.int32, x.shape, 0)
    x = x + jnp.where(row < 2, -0.5, 0.275)
    x = jnp.where(row < 3, x, 0.0)
    h = jnp.round(x * 256.0) * (1.0 / 256.0)
    rest = x - h
    m = jnp.round(rest * 65536.0) * (1.0 / 65536.0)
    l = rest - m
    a = h * h
    a1 = jnp.round(a * 256.0) * (1.0 / 256.0)
    b = 2.0 * h * rest + rest * rest
    b1 = jnp.round(b * 131072.0) * (1.0 / 131072.0)
    return row, h, m, l, (a1, a - a1, b1, b - b1)


def pair(first, second):
    return first + pltpu.roll(second, 3, 0)


def eight_rows(x):
    return jnp.concatenate([x, jnp.zeros((8 - x.shape[0], x.shape[1]), F32)], axis=0)


def cell_features(x):
    row, h, m, l, (a1, a2, b1, b2) = pieces(x)
    ones = jnp.ones_like(x)
    zero = jnp.zeros_like(x)
    return jnp.concatenate([pair(h, h), pair(h, m), pair(m, m), pair(l, l), l, pair(a1, a2),
                            pair(b1, b2), ones, ones, zero], axis=0).astype(BF16)


def station_features(x):
    row, h, m, l, (a1, a2, b1, b2) = pieces(x)
    ones = jnp.where(row < 6, 1.0, 0.0)
    soft = jnp.where(row == 6, SOFT_PIECES[0], 0.0) + jnp.where(row == 7, SOFT_PIECES[1], 0.0)
    rest = jnp.where(row == 6, SOFT_PIECES[2], 0.0)
    zero = jnp.zeros_like(x)
    h2, m2, l2 = -2.0 * h, -2.0 * m, -2.0 * l
    return jnp.concatenate([pair(h2, m2), pair(l2, h2), pair(m2, l2), pair(h2, m2), l2, ones,
                            ones, pair(a1, a2) + soft, pair(b1, b2) + rest, zero], axis=0)


def kernel(sizes, st_hbm, cell_hbm, w_hbm, m_hbm, data_hbm, model_ref, res_ref, search_ref,
           kmat, rhs, lhs, cell_v, w_v, m_all, st_all, szb, urow, acc, gacc, rb, rrow, qrow, grow,
           out1, out2, rs1, rs2, part1, part2, gather1, gather2, gmsg, gnmsg, gout, gnout, dout, din, drow,
           in_sem, st_send, st_recv, m_sem, ar_send, ar_recv1, ar_recv2, ex_send, ex_recv1, ex_recv2,
           sc_send, sc_recv, data_v):
    n_sta, n_cell, cells, width, piece, scale = sizes
    nz = n_sta // 2
    chips = nz * n_cell
    tiles = 2 * cells // LANES
    half = cells // LANES
    groups = width // 8
    high = width // LANES
    per_tile = LANES // piece
    my_sta, my_cell = lax.axis_index("sta"), lax.axis_index("cell")
    core = lax.rem(my_sta, 2)
    z = lax.div(my_sta, 2)
    chip = z * n_cell + my_cell
    partner = (z * 2 + 1 - core, my_cell)

    def peer(k):
        flat = lax.rem(chip + k, chips)
        return (lax.div(flat, n_cell) * 2 + core, lax.rem(flat, n_cell))

    def every_peer(act):
        if chips > 16 or chips & (chips - 1) or n_cell & (n_cell - 1):
            def one(k, c):
                act(peer(k))
                return c

            lax.fori_loop(1, chips, one, 0)
        else:
            for k in range(chips - 1, 0, -1):
                act((my_sta ^ (k // n_cell * 2), my_cell ^ (k % n_cell)))

    def remote(src, dst, send, recv, device):
        return pltpu.make_async_remote_copy(src_ref=src, dst_ref=dst, send_sem=send, recv_sem=recv,
                                            device_id=device, device_id_type=MESH)

    def drain(ref, sem):
        pltpu.make_async_copy(ref, ref, sem).wait()

    barrier = pltpu.get_barrier_semaphore()

    every_peer(lambda device: pl.semaphore_signal(barrier, inc=1, device_id=device, device_id_type=MESH))
    pl.semaphore_signal(barrier, inc=1, device_id=partner, device_id_type=MESH)

    first_cell = pl.multiple_of(z * 2 * cells, 2 * cells)
    first_row = pl.multiple_of(z * tiles, tiles)
    load_cells = pltpu.make_async_copy(cell_hbm.at[:, pl.ds(first_cell, 2 * cells)], cell_v, in_sem.at[0])
    load_stations = pltpu.make_async_copy(st_hbm, st_all.at[z], in_sem.at[1])
    load_weights = pltpu.make_async_copy(w_hbm.at[pl.ds(first_row, tiles)], w_v, in_sem.at[2])
    load_model = pltpu.make_async_copy(m_hbm, m_all.at[core], in_sem.at[3])
    load_cells.start()
    load_stations.start()
    load_weights.start()
    load_model.start()
    load_data = pltpu.make_async_copy(data_hbm, data_v, in_sem.at[4])
    load_data.start()

    def features(n, c):
        cols = pl.ds(pl.multiple_of(n * 512, 512), 512)
        rhs[:, cols] = cell_features(eight_rows(cell_v[:, cols]))
        return c

    load_cells.wait()
    lax.fori_loop(0, 2 * cells // 512, features, 0)

    def prepare(b):
        x = eight_rows(st_all[b])
        feats = station_features(x)
        for i in range(high):
            cols = slice(i * LANES, (i + 1) * LANES)
            lhs[cols, :] = jnp.transpose(feats[:, cols]).astype(BF16)
            zz = jnp.transpose(jnp.broadcast_to(x[2:3, cols], (LANES, LANES)))
            szb[i * 16:(i + 1) * 16] = zz.reshape(16, 8, LANES)

    block = min(2048, 2 * cells)

    def build(b, n):
        at = pl.multiple_of(n * block, block)
        r2 = jnp.dot(lhs[...], rhs[:, pl.ds(at, block)], preferred_element_type=F32)
        r2 = r2.reshape(groups, 8, block)
        cz = cell_v[2:3, pl.ds(at, block)]
        out = []
        for t in range(block // LANES):
            cols = slice(t * LANES, (t + 1) * LANES)
            inv = lax.rsqrt(r2[:, :, cols])
            dz = szb[...] - jnp.broadcast_to(cz[:, cols], (8, LANES))[None]
            out.append((dz * inv) * (inv * inv))
        kmat[pl.ds(b * groups, groups), :, pl.ds(at, block)] = jnp.concatenate(out, axis=2)

    def build_from(b, first):
        def one(n, c):
            build(b, n)
            return c

        lax.fori_loop(first, 2 * cells // block, one, 0)

    step = 8

    def forward(b, h, add):
        us = [jnp.broadcast_to(urow[pl.ds(h * half + t, 1), :], (8, LANES)) for t in range(half)]

        def some(i, c):
            for j in range(step):
                g = i * step + j
                sums = [None] * 4
                for t in range(half):
                    cols = pl.ds(pl.multiple_of(h * cells + t * LANES, LANES), LANES)
                    value = kmat[b * groups + g, :, cols] * us[t]
                    sums[t % 4] = value if sums[t % 4] is None else sums[t % 4] + value
                value = (sums[0] + sums[1]) + (sums[2] + sums[3])
                acc[b * groups + g] = value + acc[b * groups + g] if add else value
            return c

        lax.fori_loop(0, groups // step, some, 0)

    def block_rows(b):
        rows = []
        for i in range(high):
            x = acc[pl.ds(b * groups + i * 16, 16)].reshape(LANES, LANES)
            rows.append(jnp.sum(jnp.transpose(x), axis=0, keepdims=True))
        return jnp.concatenate(rows, axis=0)

    def send_rows(rows, out, rs, recv, b, which=0):
        out[b] = rows
        rs[b, chip] = rows

        every_peer(lambda device: remote(out.at[b], rs.at[b, chip], ar_send.at[which], recv.at[b],
                                         device).start())

    def broadcast(value, out, msgs, which):
        out[...] = value
        msgs[chip] = value

        every_peer(lambda device: remote(out, msgs.at[chip], sc_send.at[which], sc_recv.at[which],
                                         device).start())

    low = z < nz // 2

    def order(k):
        if nz & (nz - 1):
            return lax.rem(z + k, nz)
        return z ^ jnp.where(low & (k > 0), jnp.where(k == nz - 1, 1, k + 1), k)

    def fixed(j):
        return nz - 1 - j

    def settled(j):
        return jnp.where(j < nz - 2, nz - 1 - j, jnp.where(low, nz - 1 - j, j - nz + 2))

    load_stations.wait()
    prepare(z)

    def enter():
        pl.semaphore_wait(barrier, chips)

        def send_stations(k, c):
            other = lax.rem(z + k, nz)
            remote(st_all.at[z], st_all.at[z], st_send, st_recv.at[z], (other * 2 + core, my_cell)).start()
            return c

        lax.fori_loop(1, nz, send_stations, 0)
        remote(m_all.at[core], m_all.at[core], m_sem.at[0], m_sem.at[1], partner).start()

    load_model.wait()
    pl.when((z == nz - 1) & (z > 0))(enter)
    build(z, 0)
    pl.when((z > 0) & (z < nz - 1))(enter)
    build_from(z, 1)
    pl.when(z == 0)(enter)
    load_weights.wait()
    ws = w_v[...] * scale
    w_v[...] = ws
    drain(m_all.at[0], m_sem.at[1])
    urow[...] = ws * m_all[...].reshape(tiles, LANES)

    load_data.wait()
    data = data_v[...]
    drow[...] = jnp.zeros((high, LANES), F32)
    lane = lax.broadcasted_iota(jnp.int32, (1, LANES), 1)
    wide = jnp.where(lane < piece, jnp.concatenate([data] * per_tile, axis=1), 0.0)
    for q in range(n_cell):
        tile, at = q // per_tile, q % per_tile
        value = pltpu.roll(wide, at * piece, 1) if at else wide
        drow[tile:tile + 1, :] += jnp.where(my_cell == q, value, 0.0)

    forward(z, 0, False)
    forward(z, 1, True)

    def rest(k, c):
        b = order(k)
        drain(st_all.at[b], st_recv.at[b])
        rows = block_rows(order(k - 1)) - jnp.where(k == 1, drow[...], 0.0)
        prepare(b)
        send_rows(rows, out1, rs1, ar_recv1, order(k - 1))
        build_from(b, 0)
        forward(b, 0, False)
        forward(b, 1, True)
        return c

    lax.fori_loop(1, nz, rest, 0)
    send_rows(block_rows(order(nz - 1)), out1, rs1, ar_recv1, order(nz - 1))

    def arrive(b, rs, recv, store, sign):
        drain(rs.at[b, pl.ds(0, chips - 1)], recv.at[b])
        row = sign * jnp.sum(rs[b], axis=0)
        store[b] = row
        for i in range(high):
            x = jnp.transpose(jnp.broadcast_to(row[i:i + 1], (LANES, LANES)))
            rb[i * 16:(i + 1) * 16] = x.reshape(16, 8, LANES)

    strip = 16

    def backward(b, at):
        x = kmat[pl.ds(b * groups, groups), :, pl.ds(pl.multiple_of(at * LANES, LANES), strip * LANES)]
        return [gacc[at + t] + jnp.sum(x[:, :, t * LANES:(t + 1) * LANES] * rb[...], axis=0)
                for t in range(strip)]

    def gradient(turn, rs, recv, store, sign, part, gather, send, ex_recv, complete):
        gacc[...] = jnp.zeros((tiles, 8, LANES), F32)

        def early(j, c):
            b = turn(j)
            arrive(b, rs, recv, store, sign)

            def some(i, c):
                for t, total in enumerate(backward(b, i * strip)):
                    gacc[i * strip + t] = total
                return c

            lax.fori_loop(0, tiles // strip, some, 0)
            return c

        lax.fori_loop(0, nz - 1, early, 0)
        b = turn(nz - 1)
        arrive(b, rs, recv, store, sign)
        complete()
        for h in range(2):
            def some(i, c):
                rows = [jnp.sum(a, axis=0, keepdims=True) for a in backward(b, h * half + i * strip)]
                part[h, pl.ds(pl.multiple_of(i * strip, strip), strip)] = jnp.concatenate(rows, axis=0)
                return c

            lax.fori_loop(0, half // strip, some, 0)
            remote(part.at[h], gather.at[h], send, ex_recv.at[h], partner).start()

    gradient(settled, rs1, ar_recv1, rrow, -1.0, part1, gather1, ex_send.at[0], ex_recv1, lambda: None)
    for h in range(2):
        drain(gather1.at[h], ex_recv1.at[h])
        rows = slice(h * half, (h + 1) * half)
        g = w_v[rows] * (part1[h] + gather1[h])
        grow[rows] = g
        urow[rows] = w_v[rows] * g
        if h == 0:
            forward(fixed(0), 0, False)
            forward(fixed(1), 0, False)
    g = grow[...]
    broadcast(jnp.sum(g * g, axis=0, keepdims=True), gout, gmsg, 0)

    def image(j, c):
        b = fixed(j)

        @pl.when(j >= 2)
        def _():
            forward(b, 0, False)

        forward(b, 1, True)
        send_rows(block_rows(b), out2, rs2, ar_recv2, b, 1)
        return c

    lax.fori_loop(0, nz, image, 0)

    def send_delta():
        q = qrow[...]
        dout[...] = jnp.sum(jnp.sum(q * q, axis=0), axis=0, keepdims=True)
        remote(dout, din, sc_send.at[1], sc_recv.at[1], partner).start()

    gradient(fixed, rs2, ar_recv2, qrow, 1.0, part2, gather2, ex_send.at[1], ex_recv2, send_delta)

    def total(msgs, which):
        drain(msgs.at[pl.ds(0, chips - 1)], sc_recv.at[which])
        return jnp.sum(jnp.sum(msgs[...], axis=0), axis=1, keepdims=True)

    gamma = total(gmsg, 0)
    drain(din, sc_recv.at[1])
    alpha = gamma / jnp.sum(dout[...] + din[...], axis=1, keepdims=True)

    own = pl.ds(pl.multiple_of(core * half, half), half)
    model_ref[...] = m_all[core] + alpha * grow[own]
    new = rrow[z] - alpha * qrow[z]
    mine = jnp.zeros((1, LANES), F32)
    for q in range(n_cell):
        tile, at = q // per_tile, q % per_tile
        value = new[tile:tile + 1]
        if at:
            value = pltpu.roll(value, LANES - at * piece, 1)
        mine = jnp.where(my_cell == q, value, mine)
    res_ref[...] = mine[:, :piece]

    square = jnp.zeros((half, LANES), F32)
    for h in range(2):
        drain(gather2.at[h], ex_recv2.at[h])
        rows = slice(h * half, (h + 1) * half)
        g = grow[rows] - alpha * (w_v[rows] * (part2[h] + gather2[h]))
        urow[rows] = g
        square += g * g
    value = jnp.sum(square, axis=0, keepdims=True)
    gnout[...] = value
    gnmsg[chip] = value

    def tell(device):
        for sta in (device[0] ^ 1, device[0]):
            remote(gnout, gnmsg.at[chip], sc_send.at[2], sc_recv.at[2], (sta, device[1])).start()

    pl.when(core == 1)(lambda: every_peer(tell))
    beta = total(gnmsg, 2) / gamma
    search_ref[...] = urow[own] + beta * grow[own]

    drain(st_all.at[pl.ds(0, nz - 1)], st_send)
    drain(m_all.at[0], m_sem.at[0])
    drain(rs1.at[:, pl.ds(0, chips - 1)], ar_send.at[0])
    drain(rs2.at[:, pl.ds(0, chips - 1)], ar_send.at[1])
    drain(part1, ex_send.at[0])
    drain(part2, ex_send.at[1])
    drain(gmsg.at[pl.ds(0, chips - 1)], sc_send.at[0])
    drain(din, sc_send.at[1])

    @pl.when(core == 1)
    def _():
        for _ in range(2):
            drain(gnmsg.at[pl.ds(0, chips - 1)], sc_send.at[2])


def per_device(station_xyz, cell_xyz, cell_weight, data, model_start):
    n_sta, n_cell = lax.axis_size("sta"), lax.axis_size("cell")
    n = n_sta * n_cell
    width = station_xyz.shape[1]
    cells = model_start.shape[0]
    piece = data.shape[0]
    scale = 1.0 / math.sqrt(width * n_sta * cells * n)
    sizes = (n_sta, n_cell, cells, width, piece, scale)
    nz = n_sta // 2
    chips = nz * n_cell
    tiles, half = 2 * cells // LANES, cells // LANES
    groups, high = width // 8, width // LANES
    hbm = pl.BlockSpec(memory_space=pltpu.HBM)
    vmem = pl.BlockSpec(memory_space=pltpu.VMEM)
    spread = pltpu.VMEM((nz * groups, 8, LANES), F32)
    narrow = pltpu.VMEM((groups, 8, LANES), F32)
    lines = pltpu.VMEM((nz, high, LANES), F32)
    whole = pltpu.VMEM((nz, chips, high, LANES), F32)
    halves = pltpu.VMEM((2, half, LANES), F32)
    packed = pltpu.VMEM((tiles, LANES), F32)
    message = pltpu.VMEM((chips, 1, LANES), F32)
    row = pltpu.VMEM((1, LANES), F32)
    dma = pltpu.SemaphoreType.DMA
    model_next, residual, search = pl.pallas_call(
        functools.partial(kernel, sizes),
        out_shape=(jax.ShapeDtypeStruct((half, LANES), F32), jax.ShapeDtypeStruct((1, piece), F32),
                   jax.ShapeDtypeStruct((half, LANES), F32)),
        in_specs=[hbm] * 5,
        out_specs=(vmem, vmem, vmem),
        scratch_shapes=[
            pltpu.VMEM((nz * groups, 8, 2 * cells), F32),
            pltpu.VMEM((FEATURES, 2 * cells), BF16),
            pltpu.VMEM((width, FEATURES), BF16),
            pltpu.VMEM((3, 2 * cells), F32),
            packed, halves,
            pltpu.VMEM((nz, 3, width), F32),
            narrow, packed, spread,
            pltpu.VMEM((tiles, 8, LANES), F32),
            narrow, lines, lines, packed,
            lines, lines, whole, whole,
            halves, halves, halves, halves,
            message, message, row, row, row, row,
            pltpu.VMEM((high, LANES), F32),
            dma((5,)), dma, dma((nz,)), dma((2,)), dma((2,)), dma((nz,)), dma((nz,)),
            dma((2,)), dma((2,)), dma((2,)), dma((3,)), dma((3,)),
            pltpu.VMEM((1, piece), F32),
        ],
        compiler_params=pltpu.CompilerParams(
            collective_id=0, has_side_effects=True, vmem_limit_bytes=48 * 1024 * 1024),
    )(*[pltpu.with_memory_space_constraint(x, pltpu.HBM) for x in (station_xyz, cell_xyz, cell_weight.reshape(-1, LANES), model_start.reshape(-1, LANES),
      data.reshape(1, piece))])
    def hand(a, b, c, x, y, z):
        x[...] = a[...]
        y[...] = b[...]
        z[...] = c[...]

    model_next, residual, search = pl.pallas_call(
        hand,
        out_shape=(jax.ShapeDtypeStruct((half, LANES), F32), jax.ShapeDtypeStruct((1, piece), F32),
                   jax.ShapeDtypeStruct((half, LANES), F32)),
        in_specs=[vmem] * 3, out_specs=(vmem, vmem, vmem),
        compiler_params=pltpu.CompilerParams(vmem_limit_bytes=1024 * 1024),
    )(model_next, residual, search)
    return (model_next.reshape(cells), residual.reshape(piece), search.reshape(cells))


def solution(mesh):
    placed = (P(None, "sta"), P(None, "cell"), P("cell"), P(("sta", "cell")), P(("cell", "sta")))
    return jax.shard_map(
        per_device,
        mesh=mesh,
        in_specs=placed,
        out_specs=(P(("cell", "sta")), P(("sta", "cell")), P(("cell", "sta"))),
        check_vma=False,
    )
```

```python
import functools
import math

import jax
import jax.numpy as jnp
import numpy as np
from jax import lax
from jax.experimental import pallas as pl
from jax.experimental.pallas import tpu as pltpu
from jax.sharding import PartitionSpec as P

SOFT = float(np.float32(0.0001))


def split(value):
    out = []
    for _ in range(3):
        scale = 2.0 ** (math.floor(math.log2(value)) - 7)
        out.append(math.floor(value / scale) * scale)
        value -= out[-1]
    return out


SOFT_PIECES = split(SOFT)
LANES = 128
FEATURES = 80
MESH = pl.DeviceIdType.MESH
F32 = jnp.float32
BF16 = jnp.bfloat16


def pieces(x):
    row = lax.broadcasted_iota(jnp.int32, x.shape, 0)
    x = x + jnp.where(row < 2, -0.5, 0.275)
    x = jnp.where(row < 3, x, 0.0)
    h = jnp.round(x * 256.0) * (1.0 / 256.0)
    rest = x - h
    m = jnp.round(rest * 65536.0) * (1.0 / 65536.0)
    l = rest - m
    a = h * h
    a1 = jnp.round(a * 256.0) * (1.0 / 256.0)
    b = 2.0 * h * rest + rest * rest
    b1 = jnp.round(b * 131072.0) * (1.0 / 131072.0)
    return row, h, m, l, (a1, a - a1, b1, b - b1)


def pair(first, second):
    return first + pltpu.roll(second, 3, 0)


def eight_rows(x):
    return jnp.concatenate([x, jnp.zeros((8 - x.shape[0], x.shape[1]), F32)], axis=0)


def cell_features(x):
    row, h, m, l, (a1, a2, b1, b2) = pieces(x)
    ones = jnp.ones_like(x)
    zero = jnp.zeros_like(x)
    return jnp.concatenate([pair(h, h), pair(h, m), pair(m, m), pair(l, l), l, pair(a1, a2),
                            pair(b1, b2), ones, ones, zero], axis=0).astype(BF16)


def station_features(x):
    row, h, m, l, (a1, a2, b1, b2) = pieces(x)
    ones = jnp.where(row < 6, 1.0, 0.0)
    soft = jnp.where(row == 6, SOFT_PIECES[0], 0.0) + jnp.where(row == 7, SOFT_PIECES[1], 0.0)
    rest = jnp.where(row == 6, SOFT_PIECES[2], 0.0)
    zero = jnp.zeros_like(x)
    h2, m2, l2 = -2.0 * h, -2.0 * m, -2.0 * l
    return jnp.concatenate([pair(h2, m2), pair(l2, h2), pair(m2, l2), pair(h2, m2), l2, ones,
                            ones, pair(a1, a2) + soft, pair(b1, b2) + rest, zero], axis=0)


def kernel(sizes, st_hbm, cell_hbm, w_hbm, m_hbm, data_hbm, model_ref, res_ref, search_ref,
           kmat, rhs, lhs, cell_v, w_v, m_all, st_all, szb, urow, acc, gacc, rb, rrow, qrow, grow,
           out1, out2, rs1, rs2, part1, part2, gather1, gather2, gmsg, gnmsg, gout, gnout, dout, din,
           in_sem, st_send, st_recv, m_sem, ar_send, ar_recv1, ar_recv2, ex_send, ex_recv1, ex_recv2,
           sc_send, sc_recv, data_v):
    n_sta, n_cell, cells, width, piece, scale = sizes
    nz = n_sta // 2
    chips = nz * n_cell
    tiles = 2 * cells // LANES
    half = cells // LANES
    groups = width // 8
    high = width // LANES
    per_tile = LANES // piece
    my_sta, my_cell = lax.axis_index("sta"), lax.axis_index("cell")
    core = lax.rem(my_sta, 2)
    z = lax.div(my_sta, 2)
    chip = z * n_cell + my_cell
    partner = (z * 2 + 1 - core, my_cell)

    def peer(k):
        flat = lax.rem(chip + k, chips)
        return (lax.div(flat, n_cell) * 2 + core, lax.rem(flat, n_cell))

    def every_peer(act):
        if chips > 16 or chips & (chips - 1) or n_cell & (n_cell - 1):
            def one(k, c):
                act(peer(k))
                return c

            lax.fori_loop(1, chips, one, 0)
        else:
            for k in range(chips - 1, 0, -1):
                act((my_sta ^ (k // n_cell * 2), my_cell ^ (k % n_cell)))

    def remote(src, dst, send, recv, device):
        return pltpu.make_async_remote_copy(src_ref=src, dst_ref=dst, send_sem=send, recv_sem=recv,
                                            device_id=device, device_id_type=MESH)

    def drain(ref, sem):
        pltpu.make_async_copy(ref, ref, sem).wait()

    barrier = pltpu.get_barrier_semaphore()

    around = [(lax.rem(z + k, nz) * 2 + core, my_cell) for k in range(1, nz)]
    around += [(my_sta, lax.rem(my_cell + k, n_cell)) for k in range(1, n_cell)]
    around.append(partner)
    for device in around:
        pl.semaphore_signal(barrier, inc=1, device_id=device, device_id_type=MESH)

    first_cell = pl.multiple_of(z * 2 * cells, 2 * cells)
    first_row = pl.multiple_of(z * tiles, tiles)
    load_cells = pltpu.make_async_copy(cell_hbm.at[:, pl.ds(first_cell, 2 * cells)], cell_v, in_sem.at[0])
    load_stations = pltpu.make_async_copy(st_hbm, st_all.at[z], in_sem.at[1])
    load_weights = pltpu.make_async_copy(w_hbm.at[pl.ds(first_row, tiles)], w_v, in_sem.at[2])
    load_model = pltpu.make_async_copy(m_hbm, m_all.at[core], in_sem.at[3])
    load_stations.start()
    load_cells.start()
    load_weights.start()
    load_model.start()
    load_data = pltpu.make_async_copy(data_hbm, data_v, in_sem.at[4])
    load_data.start()

    lot = min(2048, 2 * cells)

    def features(n, c):
        cols = pl.ds(pl.multiple_of(n * lot, lot), lot)
        rhs[:, cols] = cell_features(eight_rows(cell_v[:, cols]))
        return c

    def prepare(b):
        x = eight_rows(st_all[b])
        feats = station_features(x)
        for i in range(high):
            cols = slice(i * LANES, (i + 1) * LANES)
            lhs[cols, :] = jnp.transpose(feats[:, cols]).astype(BF16)
            zz = jnp.transpose(jnp.broadcast_to(x[2:3, cols], (LANES, LANES)))
            szb[i * 16:(i + 1) * 16] = zz.reshape(16, 8, LANES)

    block = min(2048, 2 * cells)

    def build(b, n):
        at = pl.multiple_of(n * block, block)
        r2 = jnp.dot(lhs[...], rhs[:, pl.ds(at, block)], preferred_element_type=F32)
        r2 = r2.reshape(groups, 8, block)
        cz = cell_v[2:3, pl.ds(at, block)]
        out = []
        for t in range(block // LANES):
            cols = slice(t * LANES, (t + 1) * LANES)
            inv = lax.rsqrt(r2[:, :, cols])
            dz = szb[...] - jnp.broadcast_to(cz[:, cols], (8, LANES))[None]
            out.append((dz * inv) * (inv * inv))
        kmat[pl.ds(b * groups, groups), :, pl.ds(at, block)] = jnp.concatenate(out, axis=2)

    def build_from(b, first):
        def one(n, c):
            build(b, n)
            return c

        lax.fori_loop(first, 2 * cells // block, one, 0)

    step = 8

    def forward(b, h, add):
        us = [jnp.broadcast_to(urow[pl.ds(h * half + t, 1), :], (8, LANES)) for t in range(half)]

        def some(i, c):
            for j in range(step):
                g = i * step + j
                sums = [None] * 4
                for t in range(half):
                    cols = pl.ds(pl.multiple_of(h * cells + t * LANES, LANES), LANES)
                    value = kmat[b * groups + g, :, cols] * us[t]
                    sums[t % 4] = value if sums[t % 4] is None else sums[t % 4] + value
                value = (sums[0] + sums[1]) + (sums[2] + sums[3])
                acc[b * groups + g] = value + acc[b * groups + g] if add else value
            return c

        lax.fori_loop(0, groups // step, some, 0)

    def block_rows(b):
        rows = []
        for i in range(high):
            x = acc[pl.ds(b * groups + i * 16, 16)].reshape(LANES, LANES)
            rows.append(jnp.sum(jnp.transpose(x), axis=0, keepdims=True))
        return jnp.concatenate(rows, axis=0)

    def keep_rows(rows, out, rs, b):
        out[b] = rows
        rs[b, chip] = rows

    def send_kept(out, rs, recv, b, which):
        every_peer(lambda device: remote(out.at[b], rs.at[b, chip], ar_send.at[which], recv.at[b],
                                         device).start())

    def send_rows(rows, out, rs, recv, b, which=0):
        keep_rows(rows, out, rs, b)
        send_kept(out, rs, recv, b, which)

    def broadcast(value, out, msgs, which):
        out[...] = value
        msgs[chip] = value

        every_peer(lambda device: remote(out, msgs.at[chip], sc_send.at[which], sc_recv.at[which],
                                         device).start())

    low = z < nz // 2

    def order(k):
        if nz < 2 or nz & (nz - 1):
            return lax.rem(z + k, nz)
        far = nz // 2
        return jnp.where(low & (k > 0) & (k <= far), far + k - 1, z ^ jnp.where(low & (k > far), k - far, k))

    def fixed(j):
        return nz - 1 - j

    def settled(j):
        far = nz // 2
        return jnp.where(j < far, jnp.where(j + far < nz, far + j, j),
                         jnp.where(low, nz - 1 - j, j - far))

    load_stations.wait()
    prepare(z)
    load_cells.wait()
    lax.fori_loop(0, 2 * cells // lot, features, 0)

    def enter():
        pl.semaphore_wait(barrier, len(around))

        def send_stations(k, c):
            other = lax.rem(z + k, nz)
            remote(st_all.at[z], st_all.at[z], st_send, st_recv.at[z], (other * 2 + core, my_cell)).start()
            return c

        lax.fori_loop(1, nz, send_stations, 0)
        remote(m_all.at[core], m_all.at[core], m_sem.at[0], m_sem.at[1], partner).start()

    load_model.wait()
    pl.when((z == nz - 1) & (z > 0))(enter)
    build(z, 0)
    pl.when((z > 0) & (z < nz - 1))(enter)
    build_from(z, 1)
    pl.when(z == 0)(enter)
    load_weights.wait()
    ws = w_v[...] * scale
    w_v[...] = ws
    drain(m_all.at[0], m_sem.at[1])
    urow[...] = ws * m_all[...].reshape(tiles, LANES)

    forward(z, 0, False)
    forward(z, 1, True)

    def stations_of(k):
        drain(st_all.at[order(k)], st_recv.at[order(k)])

    def own_rows():
        load_data.wait()
        lane = lax.broadcasted_iota(jnp.int32, (1, LANES), 1)
        wide = jnp.where(lane < piece, jnp.concatenate([data_v[...]] * per_tile, axis=1), 0.0)
        rows = [jnp.zeros((1, LANES), F32)] * high
        for q in range(n_cell):
            tile, at = q // per_tile, q % per_tile
            value = pltpu.roll(wide, at * piece, 1) if at else wide
            rows[tile] = jnp.where(my_cell == q, value, rows[tile])
        return block_rows(z) - jnp.concatenate(rows, axis=0)

    if nz > 1:
        stations_of(1)
        keep_rows(own_rows(), out1, rs1, z)
        prepare(order(1))
        build_from(order(1), 0)
        forward(order(1), 0, False)
        forward(order(1), 1, True)
    else:
        keep_rows(own_rows(), out1, rs1, z)

    def rest(k, c):
        b = order(k)

        @pl.when(k == 2)
        def _():
            for i in range(2, nz):
                stations_of(i)
            send_kept(out1, rs1, ar_recv1, z, 0)

        rows = block_rows(order(k - 1))
        prepare(b)
        send_rows(rows, out1, rs1, ar_recv1, order(k - 1))
        build_from(b, 0)
        forward(b, 0, False)
        forward(b, 1, True)
        return c

    lax.fori_loop(2, nz, rest, 0)
    if nz < 3:
        send_kept(out1, rs1, ar_recv1, z, 0)
    if nz > 1:
        send_rows(block_rows(order(nz - 1)), out1, rs1, ar_recv1, order(nz - 1))

    def arrive(b, rs, recv, store, sign):
        drain(rs.at[b, pl.ds(0, chips - 1)], recv.at[b])
        row = sign * jnp.sum(rs[b], axis=0)
        store[b] = row
        for i in range(high):
            x = jnp.transpose(jnp.broadcast_to(row[i:i + 1], (LANES, LANES)))
            rb[i * 16:(i + 1) * 16] = x.reshape(16, 8, LANES)

    strip = 16

    def backward(b, at):
        x = kmat[pl.ds(b * groups, groups), :, pl.ds(pl.multiple_of(at * LANES, LANES), strip * LANES)]
        return [gacc[at + t] + jnp.sum(x[:, :, t * LANES:(t + 1) * LANES] * rb[...], axis=0)
                for t in range(strip)]

    def gradient(turn, rs, recv, store, sign, part, gather, send, ex_recv, complete):
        gacc[...] = jnp.zeros((tiles, 8, LANES), F32)

        def early(j, c):
            b = turn(j)
            arrive(b, rs, recv, store, sign)

            def some(i, c):
                for t, total in enumerate(backward(b, i * strip)):
                    gacc[i * strip + t] = total
                return c

            lax.fori_loop(0, tiles // strip, some, 0)
            return c

        lax.fori_loop(0, nz - 1, early, 0)
        b = turn(nz - 1)
        arrive(b, rs, recv, store, sign)
        complete()
        for h in range(2):
            def some(i, c):
                rows = [jnp.sum(a, axis=0, keepdims=True) for a in backward(b, h * half + i * strip)]
                part[h, pl.ds(pl.multiple_of(i * strip, strip), strip)] = jnp.concatenate(rows, axis=0)
                return c

            lax.fori_loop(0, half // strip, some, 0)
            remote(part.at[h], gather.at[h], send, ex_recv.at[h], partner).start()

    gradient(settled, rs1, ar_recv1, rrow, -1.0, part1, gather1, ex_send.at[0], ex_recv1, lambda: None)
    for h in range(2):
        drain(gather1.at[h], ex_recv1.at[h])
        rows = slice(h * half, (h + 1) * half)
        g = w_v[rows] * (part1[h] + gather1[h])
        grow[rows] = g
        urow[rows] = w_v[rows] * g
        if h == 0:
            forward(fixed(0), 0, False)
            forward(fixed(1), 0, False)
    g = grow[...]
    broadcast(jnp.sum(g * g, axis=0, keepdims=True), gout, gmsg, 0)

    def image(j, c):
        b = fixed(j)

        @pl.when(j >= 2)
        def _():
            forward(b, 0, False)

        forward(b, 1, True)
        send_rows(block_rows(b), out2, rs2, ar_recv2, b, 1)
        return c

    lax.fori_loop(0, nz, image, 0)

    def send_delta():
        q = qrow[...]
        dout[...] = jnp.sum(jnp.sum(q * q, axis=0), axis=0, keepdims=True)
        remote(dout, din, sc_send.at[1], sc_recv.at[1], partner).start()

    gradient(fixed, rs2, ar_recv2, qrow, 1.0, part2, gather2, ex_send.at[1], ex_recv2, send_delta)

    def total(msgs, which):
        drain(msgs.at[pl.ds(0, chips - 1)], sc_recv.at[which])
        return jnp.sum(jnp.sum(msgs[...], axis=0), axis=1, keepdims=True)

    gamma = total(gmsg, 0)
    drain(din, sc_recv.at[1])
    alpha = gamma / jnp.sum(dout[...] + din[...], axis=1, keepdims=True)

    own = pl.ds(pl.multiple_of(core * half, half), half)
    model_ref[...] = m_all[core] + alpha * grow[own]
    new = rrow[z] - alpha * qrow[z]
    mine = jnp.zeros((1, LANES), F32)
    for q in range(n_cell):
        tile, at = q // per_tile, q % per_tile
        value = new[tile:tile + 1]
        if at:
            value = pltpu.roll(value, LANES - at * piece, 1)
        mine = jnp.where(my_cell == q, value, mine)
    res_ref[...] = mine[:, :piece]

    square = jnp.zeros((half, LANES), F32)
    for h in range(2):
        drain(gather2.at[h], ex_recv2.at[h])
        rows = slice(h * half, (h + 1) * half)
        g = grow[rows] - alpha * (w_v[rows] * (part2[h] + gather2[h]))
        urow[rows] = g
        square += g * g
    value = jnp.sum(square, axis=0, keepdims=True)
    gnout[...] = value
    gnmsg[chip] = value

    def tell(device):
        for sta in (device[0] ^ 1, device[0]):
            remote(gnout, gnmsg.at[chip], sc_send.at[2], sc_recv.at[2], (sta, device[1])).start()

    pl.when(core == 1)(lambda: every_peer(tell))
    beta = total(gnmsg, 2) / gamma
    search_ref[...] = urow[own] + beta * grow[own]

    drain(st_all.at[pl.ds(0, nz - 1)], st_send)
    drain(m_all.at[0], m_sem.at[0])
    drain(rs1.at[:, pl.ds(0, chips - 1)], ar_send.at[0])
    drain(rs2.at[:, pl.ds(0, chips - 1)], ar_send.at[1])
    drain(part1, ex_send.at[0])
    drain(part2, ex_send.at[1])
    drain(gmsg.at[pl.ds(0, chips - 1)], sc_send.at[0])
    drain(din, sc_send.at[1])

    @pl.when(core == 1)
    def _():
        for _ in range(2):
            drain(gnmsg.at[pl.ds(0, chips - 1)], sc_send.at[2])


def per_device(station_xyz, cell_xyz, cell_weight, data, model_start):
    n_sta, n_cell = lax.axis_size("sta"), lax.axis_size("cell")
    n = n_sta * n_cell
    width = station_xyz.shape[1]
    cells = model_start.shape[0]
    piece = data.shape[0]
    scale = 1.0 / math.sqrt(width * n_sta * cells * n)
    sizes = (n_sta, n_cell, cells, width, piece, scale)
    nz = n_sta // 2
    chips = nz * n_cell
    tiles, half = 2 * cells // LANES, cells // LANES
    groups, high = width // 8, width // LANES
    hbm = pl.BlockSpec(memory_space=pltpu.HBM)
    vmem = pl.BlockSpec(memory_space=pltpu.VMEM)
    spread = pltpu.VMEM((nz * groups, 8, LANES), F32)
    narrow = pltpu.VMEM((groups, 8, LANES), F32)
    lines = pltpu.VMEM((nz, high, LANES), F32)
    whole = pltpu.VMEM((nz, chips, high, LANES), F32)
    halves = pltpu.VMEM((2, half, LANES), F32)
    packed = pltpu.VMEM((tiles, LANES), F32)
    message = pltpu.VMEM((chips, 1, LANES), F32)
    row = pltpu.VMEM((1, LANES), F32)
    dma = pltpu.SemaphoreType.DMA
    model_next, residual, search = pl.pallas_call(
        functools.partial(kernel, sizes),
        out_shape=(jax.ShapeDtypeStruct((half, LANES), F32), jax.ShapeDtypeStruct((1, piece), F32),
                   jax.ShapeDtypeStruct((half, LANES), F32)),
        in_specs=[hbm] * 5,
        out_specs=(vmem, vmem, vmem),
        scratch_shapes=[
            pltpu.VMEM((nz * groups, 8, 2 * cells), F32),
            pltpu.VMEM((FEATURES, 2 * cells), BF16),
            pltpu.VMEM((width, FEATURES), BF16),
            pltpu.VMEM((3, 2 * cells), F32),
            packed, halves,
            pltpu.VMEM((nz, 3, width), F32),
            narrow, packed, spread,
            pltpu.VMEM((tiles, 8, LANES), F32),
            narrow, lines, lines, packed,
            lines, lines, whole, whole,
            halves, halves, halves, halves,
            message, message, row, row, row, row,
            dma((5,)), dma, dma((nz,)), dma((2,)), dma((2,)), dma((nz,)), dma((nz,)),
            dma((2,)), dma((2,)), dma((2,)), dma((3,)), dma((3,)),
            pltpu.VMEM((1, piece), F32),
        ],
        compiler_params=pltpu.CompilerParams(
            collective_id=0, has_side_effects=True, vmem_limit_bytes=48 * 1024 * 1024),
    )(*[pltpu.with_memory_space_constraint(x, pltpu.HBM) for x in (station_xyz, cell_xyz, cell_weight.reshape(-1, LANES), model_start.reshape(-1, LANES),
      data.reshape(1, piece))])
    def hand(a, b, c, x, y, z):
        x[...] = a[...]
        y[...] = b[...]
        z[...] = c[...]

    model_next, residual, search = pl.pallas_call(
        hand,
        out_shape=(jax.ShapeDtypeStruct((half, LANES), F32), jax.ShapeDtypeStruct((1, piece), F32),
                   jax.ShapeDtypeStruct((half, LANES), F32)),
        in_specs=[vmem] * 3, out_specs=(vmem, vmem, vmem),
        compiler_params=pltpu.CompilerParams(vmem_limit_bytes=1024 * 1024),
    )(model_next, residual, search)
    return (model_next.reshape(cells), residual.reshape(piece), search.reshape(cells))


def solution(mesh):
    placed = (P(None, "sta"), P(None, "cell"), P("cell"), P(("sta", "cell")), P(("cell", "sta")))
    return jax.shard_map(
        per_device,
        mesh=mesh,
        in_specs=placed,
        out_specs=(P(("cell", "sta")), P(("sta", "cell")), P(("cell", "sta"))),
        check_vma=False,
    )
```

```python
import functools
import math

import jax
import jax.numpy as jnp
import numpy as np
from jax import lax
from jax.experimental import pallas as pl
from jax.experimental.pallas import tpu as pltpu
from jax.sharding import PartitionSpec as P

SOFT = float(np.float32(0.0001))


def split(value):
    out = []
    for _ in range(3):
        scale = 2.0 ** (math.floor(math.log2(value)) - 7)
        out.append(math.floor(value / scale) * scale)
        value -= out[-1]
    return out


SOFT_PIECES = split(SOFT)
LANES = 128
FEATURES = 80
MESH = pl.DeviceIdType.MESH
F32 = jnp.float32
BF16 = jnp.bfloat16


def pieces(x):
    row = lax.broadcasted_iota(jnp.int32, x.shape, 0)
    x = x + jnp.where(row < 2, -0.5, 0.275)
    x = jnp.where(row < 3, x, 0.0)
    h = jnp.round(x * 256.0) * (1.0 / 256.0)
    rest = x - h
    m = jnp.round(rest * 65536.0) * (1.0 / 65536.0)
    l = rest - m
    a = h * h
    a1 = jnp.round(a * 256.0) * (1.0 / 256.0)
    b = 2.0 * h * rest + rest * rest
    b1 = jnp.round(b * 131072.0) * (1.0 / 131072.0)
    return row, h, m, l, (a1, a - a1, b1, b - b1)


def pair(first, second):
    return first + pltpu.roll(second, 3, 0)


def eight_rows(x):
    return jnp.concatenate([x, jnp.zeros((8 - x.shape[0], x.shape[1]), F32)], axis=0)


def cell_features(x):
    row, h, m, l, (a1, a2, b1, b2) = pieces(x)
    ones = jnp.ones_like(x)
    zero = jnp.zeros_like(x)
    return jnp.concatenate([pair(h, h), pair(h, m), pair(m, m), pair(l, l), l, pair(a1, a2),
                            pair(b1, b2), ones, ones, zero], axis=0).astype(BF16)


def station_features(x):
    row, h, m, l, (a1, a2, b1, b2) = pieces(x)
    ones = jnp.where(row < 6, 1.0, 0.0)
    soft = jnp.where(row == 6, SOFT_PIECES[0], 0.0) + jnp.where(row == 7, SOFT_PIECES[1], 0.0)
    rest = jnp.where(row == 6, SOFT_PIECES[2], 0.0)
    zero = jnp.zeros_like(x)
    h2, m2, l2 = -2.0 * h, -2.0 * m, -2.0 * l
    return jnp.concatenate([pair(h2, m2), pair(l2, h2), pair(m2, l2), pair(h2, m2), l2, ones,
                            ones, pair(a1, a2) + soft, pair(b1, b2) + rest, zero], axis=0)


def kernel(sizes, st_hbm, cell_hbm, w_hbm, m_hbm, data_hbm, model_ref, res_ref, search_ref,
           kmat, rhs, lhs, cell_v, w_v, m_all, st_all, szb, urow, acc, gacc, rb, rrow, qrow, grow,
           out1, out2, rs1, rs2, part1, part2, gather1, gather2, gmsg, gnmsg, gout, gnout, dout, din,
           in_sem, st_send, st_recv, m_sem, ar_send, ar_recv1, ar_recv2, ex_send, ex_recv1, ex_recv2,
           sc_send, sc_recv, data_v):
    n_sta, n_cell, cells, width, piece, scale = sizes
    nz = n_sta // 2
    chips = nz * n_cell
    tiles = 2 * cells // LANES
    half = cells // LANES
    groups = width // 8
    high = width // LANES
    per_tile = LANES // piece
    my_sta, my_cell = lax.axis_index("sta"), lax.axis_index("cell")
    core = lax.rem(my_sta, 2)
    z = lax.div(my_sta, 2)
    chip = z * n_cell + my_cell
    partner = (z * 2 + 1 - core, my_cell)

    def peer(k):
        flat = lax.rem(chip + k, chips)
        return (lax.div(flat, n_cell) * 2 + core, lax.rem(flat, n_cell))

    def every_peer(act):
        if chips > 16 or chips & (chips - 1) or n_cell & (n_cell - 1):
            def one(k, c):
                act(peer(k))
                return c

            lax.fori_loop(1, chips, one, 0)
        else:
            for k in range(chips - 1, 0, -1):
                act((my_sta ^ (k // n_cell * 2), my_cell ^ (k % n_cell)))

    def remote(src, dst, send, recv, device):
        return pltpu.make_async_remote_copy(src_ref=src, dst_ref=dst, send_sem=send, recv_sem=recv,
                                            device_id=device, device_id_type=MESH)

    def drain(ref, sem):
        pltpu.make_async_copy(ref, ref, sem).wait()

    barrier = pltpu.get_barrier_semaphore()

    around = [(lax.rem(z + k, nz) * 2 + core, my_cell) for k in range(1, nz)]
    around += [(my_sta, lax.rem(my_cell + k, n_cell)) for k in range(1, n_cell)]
    around.append(partner)
    for device in around:
        pl.semaphore_signal(barrier, inc=1, device_id=device, device_id_type=MESH)

    first_cell = pl.multiple_of(z * 2 * cells, 2 * cells)
    first_row = pl.multiple_of(z * tiles, tiles)
    load_cells = pltpu.make_async_copy(cell_hbm.at[:, pl.ds(first_cell, 2 * cells)], cell_v, in_sem.at[0])
    load_stations = pltpu.make_async_copy(st_hbm, st_all.at[z], in_sem.at[1])
    load_weights = pltpu.make_async_copy(w_hbm.at[pl.ds(first_row, tiles)], w_v, in_sem.at[2])
    load_model = pltpu.make_async_copy(m_hbm, m_all.at[core], in_sem.at[3])
    load_stations.start()
    load_cells.start()
    load_weights.start()
    load_model.start()
    load_data = pltpu.make_async_copy(data_hbm, data_v, in_sem.at[4])
    load_data.start()

    lot = min(2048, 2 * cells)

    def features(n, c):
        cols = pl.ds(pl.multiple_of(n * lot, lot), lot)
        rhs[:, cols] = cell_features(eight_rows(cell_v[:, cols]))
        return c

    def prepare(b):
        x = eight_rows(st_all[b])
        feats = station_features(x)
        for i in range(high):
            cols = slice(i * LANES, (i + 1) * LANES)
            lhs[cols, :] = jnp.transpose(feats[:, cols]).astype(BF16)
            zz = jnp.transpose(jnp.broadcast_to(x[2:3, cols], (LANES, LANES)))
            szb[i * 16:(i + 1) * 16] = zz.reshape(16, 8, LANES)

    block = min(2048, 2 * cells)

    def build(b, n):
        at = pl.multiple_of(n * block, block)
        r2 = jnp.dot(lhs[...], rhs[:, pl.ds(at, block)], preferred_element_type=F32)
        r2 = r2.reshape(groups, 8, block)
        cz = cell_v[2:3, pl.ds(at, block)]
        out = []
        for t in range(block // LANES):
            cols = slice(t * LANES, (t + 1) * LANES)
            inv = lax.rsqrt(r2[:, :, cols])
            dz = szb[...] - jnp.broadcast_to(cz[:, cols], (8, LANES))[None]
            out.append((dz * inv) * (inv * inv))
        kmat[pl.ds(b * groups, groups), :, pl.ds(at, block)] = jnp.concatenate(out, axis=2)

    def build_from(b, first):
        def one(n, c):
            build(b, n)
            return c

        lax.fori_loop(first, 2 * cells // block, one, 0)

    step = 8

    def forward(b, h, add):
        us = [jnp.broadcast_to(urow[pl.ds(h * half + t, 1), :], (8, LANES)) for t in range(half)]

        def some(i, c):
            for j in range(step):
                g = i * step + j
                sums = [None] * 4
                for t in range(half):
                    cols = pl.ds(pl.multiple_of(h * cells + t * LANES, LANES), LANES)
                    value = kmat[b * groups + g, :, cols] * us[t]
                    sums[t % 4] = value if sums[t % 4] is None else sums[t % 4] + value
                value = (sums[0] + sums[1]) + (sums[2] + sums[3])
                acc[b * groups + g] = value + acc[b * groups + g] if add else value
            return c

        lax.fori_loop(0, groups // step, some, 0)

    def block_rows(b):
        rows = []
        for i in range(high):
            x = acc[pl.ds(b * groups + i * 16, 16)].reshape(LANES, LANES)
            rows.append(jnp.sum(jnp.transpose(x), axis=0, keepdims=True))
        return jnp.concatenate(rows, axis=0)

    def keep_rows(rows, out, rs, b):
        out[b] = rows
        rs[b, chip] = rows

    def send_kept(out, rs, recv, b, which):
        every_peer(lambda device: remote(out.at[b], rs.at[b, chip], ar_send.at[which], recv.at[b],
                                         device).start())

    def send_rows(rows, out, rs, recv, b, which=0):
        keep_rows(rows, out, rs, b)
        send_kept(out, rs, recv, b, which)

    def broadcast(value, out, msgs, which):
        out[...] = value
        msgs[chip] = value

        every_peer(lambda device: remote(out, msgs.at[chip], sc_send.at[which], sc_recv.at[which],
                                         device).start())

    low = z < nz // 2

    def order(k):
        if nz < 2 or nz & (nz - 1):
            return lax.rem(z + k, nz)
        far = nz // 2
        return jnp.where(low & (k > 0) & (k <= far), far + k - 1, z ^ jnp.where(low & (k > far), k - far, k))

    def fixed(j):
        return nz - 1 - j

    def settled(j):
        far = nz // 2
        return jnp.where(j < far, jnp.where(j + far < nz, far + j, j),
                         jnp.where(low, nz - 1 - j, j - far))

    load_stations.wait()
    prepare(z)
    load_cells.wait()
    lax.fori_loop(0, 2 * cells // lot, features, 0)

    def enter():
        pl.semaphore_wait(barrier, len(around))

        def send_stations(k, c):
            other = lax.rem(z + k, nz)
            remote(st_all.at[z], st_all.at[z], st_send, st_recv.at[z], (other * 2 + core, my_cell)).start()
            return c

        lax.fori_loop(1, nz, send_stations, 0)
        remote(m_all.at[core], m_all.at[core], m_sem.at[0], m_sem.at[1], partner).start()

    load_model.wait()
    pl.when((z == nz - 1) & (z > 0))(enter)
    build(z, 0)
    pl.when((z > 0) & (z < nz - 1))(enter)
    build_from(z, 1)
    pl.when(z == 0)(enter)
    load_weights.wait()
    ws = w_v[...] * scale
    w_v[...] = ws
    drain(m_all.at[0], m_sem.at[1])
    urow[...] = ws * m_all[...].reshape(tiles, LANES)

    forward(z, 0, False)
    forward(z, 1, True)

    def stations_of(k):
        drain(st_all.at[order(k)], st_recv.at[order(k)])

    def own_rows():
        load_data.wait()
        lane = lax.broadcasted_iota(jnp.int32, (1, LANES), 1)
        wide = jnp.where(lane < piece, jnp.concatenate([data_v[...]] * per_tile, axis=1), 0.0)
        rows = [jnp.zeros((1, LANES), F32)] * high
        for q in range(n_cell):
            tile, at = q // per_tile, q % per_tile
            value = pltpu.roll(wide, at * piece, 1) if at else wide
            rows[tile] = jnp.where(my_cell == q, value, rows[tile])
        return block_rows(z) - jnp.concatenate(rows, axis=0)

    if nz > 1:
        stations_of(1)
        keep_rows(own_rows(), out1, rs1, z)
        prepare(order(1))
        build_from(order(1), 0)
        forward(order(1), 0, False)
        forward(order(1), 1, True)
    else:
        keep_rows(own_rows(), out1, rs1, z)

    def rest(k, c):
        b = order(k)

        @pl.when(k == 2)
        def _():
            for i in range(2, nz):
                stations_of(i)
            send_kept(out1, rs1, ar_recv1, z, 0)

        rows = block_rows(order(k - 1))
        prepare(b)
        send_rows(rows, out1, rs1, ar_recv1, order(k - 1))
        build_from(b, 0)
        forward(b, 0, False)
        forward(b, 1, True)
        return c

    lax.fori_loop(2, nz, rest, 0)
    if nz < 3:
        send_kept(out1, rs1, ar_recv1, z, 0)
    if nz > 1:
        send_rows(block_rows(order(nz - 1)), out1, rs1, ar_recv1, order(nz - 1))

    def arrive(b, rs, recv, store, sign):
        drain(rs.at[b, pl.ds(0, chips - 1)], recv.at[b])
        row = sign * jnp.sum(rs[b], axis=0)
        store[b] = row
        for i in range(high):
            x = jnp.transpose(jnp.broadcast_to(row[i:i + 1], (LANES, LANES)))
            rb[i * 16:(i + 1) * 16] = x.reshape(16, 8, LANES)

    strip = 16

    def backward(b, at):
        x = kmat[pl.ds(b * groups, groups), :, pl.ds(pl.multiple_of(at * LANES, LANES), strip * LANES)]
        return [gacc[at + t] + jnp.sum(x[:, :, t * LANES:(t + 1) * LANES] * rb[...], axis=0)
                for t in range(strip)]

    def gradient(turn, rs, recv, store, sign, part, gather, send, ex_recv, complete):
        gacc[...] = jnp.zeros((tiles, 8, LANES), F32)

        def early(j, c):
            b = turn(j)
            arrive(b, rs, recv, store, sign)

            def some(i, c):
                for t, total in enumerate(backward(b, i * strip)):
                    gacc[i * strip + t] = total
                return c

            lax.fori_loop(0, tiles // strip, some, 0)
            return c

        lax.fori_loop(0, nz - 1, early, 0)
        b = turn(nz - 1)
        arrive(b, rs, recv, store, sign)
        complete()
        for h in range(2):
            def some(i, c):
                rows = [jnp.sum(a, axis=0, keepdims=True) for a in backward(b, h * half + i * strip)]
                part[h, pl.ds(pl.multiple_of(i * strip, strip), strip)] = jnp.concatenate(rows, axis=0)
                return c

            lax.fori_loop(0, half // strip, some, 0)
            remote(part.at[h], gather.at[h], send, ex_recv.at[h], partner).start()

    gradient(settled, rs1, ar_recv1, rrow, -1.0, part1, gather1, ex_send.at[0], ex_recv1, lambda: None)
    for h in range(2):
        drain(gather1.at[h], ex_recv1.at[h])
        rows = slice(h * half, (h + 1) * half)
        g = w_v[rows] * (part1[h] + gather1[h])
        grow[rows] = g
        urow[rows] = w_v[rows] * g
        if h == 0:
            forward(fixed(0), 0, False)
    def image(j, c):
        b = fixed(j)

        @pl.when(j >= 1)
        def _():
            forward(b, 0, False)

        forward(b, 1, True)
        send_rows(block_rows(b), out2, rs2, ar_recv2, b, 1)
        return c

    lax.fori_loop(0, nz, image, 0)
    g = grow[...]
    broadcast(jnp.sum(g * g, axis=0, keepdims=True), gout, gmsg, 0)

    def send_delta():
        q = qrow[...]
        dout[...] = jnp.sum(jnp.sum(q * q, axis=0), axis=0, keepdims=True)
        remote(dout, din, sc_send.at[1], sc_recv.at[1], partner).start()

    gradient(fixed, rs2, ar_recv2, qrow, 1.0, part2, gather2, ex_send.at[1], ex_recv2, send_delta)

    def total(msgs, which):
        drain(msgs.at[pl.ds(0, chips - 1)], sc_recv.at[which])
        return jnp.sum(jnp.sum(msgs[...], axis=0), axis=1, keepdims=True)

    gamma = total(gmsg, 0)
    drain(din, sc_recv.at[1])
    alpha = gamma / jnp.sum(dout[...] + din[...], axis=1, keepdims=True)

    own = pl.ds(pl.multiple_of(core * half, half), half)
    model_ref[...] = m_all[core] + alpha * grow[own]
    new = rrow[z] - alpha * qrow[z]
    mine = jnp.zeros((1, LANES), F32)
    for q in range(n_cell):
        tile, at = q // per_tile, q % per_tile
        value = new[tile:tile + 1]
        if at:
            value = pltpu.roll(value, LANES - at * piece, 1)
        mine = jnp.where(my_cell == q, value, mine)
    res_ref[...] = mine[:, :piece]

    square = jnp.zeros((half, LANES), F32)
    for h in range(2):
        drain(gather2.at[h], ex_recv2.at[h])
        rows = slice(h * half, (h + 1) * half)
        g = grow[rows] - alpha * (w_v[rows] * (part2[h] + gather2[h]))
        urow[rows] = g
        square += g * g
    value = jnp.sum(square, axis=0, keepdims=True)
    gnout[...] = value
    gnmsg[chip] = value

    def tell(device):
        for sta in (device[0] ^ 1, device[0]):
            remote(gnout, gnmsg.at[chip], sc_send.at[2], sc_recv.at[2], (sta, device[1])).start()

    pl.when(core == 1)(lambda: every_peer(tell))
    beta = total(gnmsg, 2) / gamma
    search_ref[...] = urow[own] + beta * grow[own]

    drain(st_all.at[pl.ds(0, nz - 1)], st_send)
    drain(m_all.at[0], m_sem.at[0])
    drain(rs1.at[:, pl.ds(0, chips - 1)], ar_send.at[0])
    drain(rs2.at[:, pl.ds(0, chips - 1)], ar_send.at[1])
    drain(part1, ex_send.at[0])
    drain(part2, ex_send.at[1])
    drain(gmsg.at[pl.ds(0, chips - 1)], sc_send.at[0])
    drain(din, sc_send.at[1])

    @pl.when(core == 1)
    def _():
        for _ in range(2):
            drain(gnmsg.at[pl.ds(0, chips - 1)], sc_send.at[2])


def per_device(station_xyz, cell_xyz, cell_weight, data, model_start):
    n_sta, n_cell = lax.axis_size("sta"), lax.axis_size("cell")
    n = n_sta * n_cell
    width = station_xyz.shape[1]
    cells = model_start.shape[0]
    piece = data.shape[0]
    scale = 1.0 / math.sqrt(width * n_sta * cells * n)
    sizes = (n_sta, n_cell, cells, width, piece, scale)
    nz = n_sta // 2
    chips = nz * n_cell
    tiles, half = 2 * cells // LANES, cells // LANES
    groups, high = width // 8, width // LANES
    hbm = pl.BlockSpec(memory_space=pltpu.HBM)
    vmem = pl.BlockSpec(memory_space=pltpu.VMEM)
    spread = pltpu.VMEM((nz * groups, 8, LANES), F32)
    narrow = pltpu.VMEM((groups, 8, LANES), F32)
    lines = pltpu.VMEM((nz, high, LANES), F32)
    whole = pltpu.VMEM((nz, chips, high, LANES), F32)
    halves = pltpu.VMEM((2, half, LANES), F32)
    packed = pltpu.VMEM((tiles, LANES), F32)
    message = pltpu.VMEM((chips, 1, LANES), F32)
    row = pltpu.VMEM((1, LANES), F32)
    dma = pltpu.SemaphoreType.DMA
    model_next, residual, search = pl.pallas_call(
        functools.partial(kernel, sizes),
        out_shape=(jax.ShapeDtypeStruct((half, LANES), F32), jax.ShapeDtypeStruct((1, piece), F32),
                   jax.ShapeDtypeStruct((half, LANES), F32)),
        in_specs=[hbm] * 5,
        out_specs=(vmem, vmem, vmem),
        scratch_shapes=[
            pltpu.VMEM((nz * groups, 8, 2 * cells), F32),
            pltpu.VMEM((FEATURES, 2 * cells), BF16),
            pltpu.VMEM((width, FEATURES), BF16),
            pltpu.VMEM((3, 2 * cells), F32),
            packed, halves,
            pltpu.VMEM((nz, 3, width), F32),
            narrow, packed, spread,
            pltpu.VMEM((tiles, 8, LANES), F32),
            narrow, lines, lines, packed,
            lines, lines, whole, whole,
            halves, halves, halves, halves,
            message, message, row, row, row, row,
            dma((5,)), dma, dma((nz,)), dma((2,)), dma((2,)), dma((nz,)), dma((nz,)),
            dma((2,)), dma((2,)), dma((2,)), dma((3,)), dma((3,)),
            pltpu.VMEM((1, piece), F32),
        ],
        compiler_params=pltpu.CompilerParams(
            collective_id=0, has_side_effects=True, vmem_limit_bytes=48 * 1024 * 1024),
    )(*[pltpu.with_memory_space_constraint(x, pltpu.HBM) for x in (station_xyz, cell_xyz, cell_weight.reshape(-1, LANES), model_start.reshape(-1, LANES),
      data.reshape(1, piece))])
    def hand(a, b, c, x, y, z):
        x[...] = a[...]
        y[...] = b[...]
        z[...] = c[...]

    model_next, residual, search = pl.pallas_call(
        hand,
        out_shape=(jax.ShapeDtypeStruct((half, LANES), F32), jax.ShapeDtypeStruct((1, piece), F32),
                   jax.ShapeDtypeStruct((half, LANES), F32)),
        in_specs=[vmem] * 3, out_specs=(vmem, vmem, vmem),
        compiler_params=pltpu.CompilerParams(vmem_limit_bytes=1024 * 1024),
    )(model_next, residual, search)
    return (model_next.reshape(cells), residual.reshape(piece), search.reshape(cells))


def solution(mesh):
    placed = (P(None, "sta"), P(None, "cell"), P("cell"), P(("sta", "cell")), P(("cell", "sta")))
    return jax.shard_map(
        per_device,
        mesh=mesh,
        in_specs=placed,
        out_specs=(P(("cell", "sta")), P(("sta", "cell")), P(("cell", "sta"))),
        check_vma=False,
    )
```

```python
import functools
import math

import jax
import jax.numpy as jnp
import numpy as np
from jax import lax
from jax.experimental import pallas as pl
from jax.experimental.pallas import tpu as pltpu
from jax.sharding import PartitionSpec as P

SOFT = float(np.float32(0.0001))


def split(value):
    out = []
    for _ in range(3):
        scale = 2.0 ** (math.floor(math.log2(value)) - 7)
        out.append(math.floor(value / scale) * scale)
        value -= out[-1]
    return out


SOFT_PIECES = split(SOFT)
LANES = 128
FEATURES = 80
MESH = pl.DeviceIdType.MESH
F32 = jnp.float32
BF16 = jnp.bfloat16


def pieces(x):
    row = lax.broadcasted_iota(jnp.int32, x.shape, 0)
    x = x + jnp.where(row < 2, -0.5, 0.275)
    x = jnp.where(row < 3, x, 0.0)
    h = jnp.round(x * 256.0) * (1.0 / 256.0)
    rest = x - h
    m = jnp.round(rest * 65536.0) * (1.0 / 65536.0)
    l = rest - m
    a = h * h
    a1 = jnp.round(a * 256.0) * (1.0 / 256.0)
    b = 2.0 * h * rest + rest * rest
    b1 = jnp.round(b * 131072.0) * (1.0 / 131072.0)
    return row, h, m, l, (a1, a - a1, b1, b - b1)


def pair(first, second):
    return first + pltpu.roll(second, 3, 0)


def eight_rows(x):
    return jnp.concatenate([x, jnp.zeros((8 - x.shape[0], x.shape[1]), F32)], axis=0)


def cell_features(x):
    row, h, m, l, (a1, a2, b1, b2) = pieces(x)
    ones = jnp.ones_like(x)
    zero = jnp.zeros_like(x)
    return jnp.concatenate([pair(h, h), pair(h, m), pair(m, m), pair(l, l), l, pair(a1, a2),
                            pair(b1, b2), ones, ones, zero], axis=0).astype(BF16)


def station_features(x):
    row, h, m, l, (a1, a2, b1, b2) = pieces(x)
    ones = jnp.where(row < 6, 1.0, 0.0)
    soft = jnp.where(row == 6, SOFT_PIECES[0], 0.0) + jnp.where(row == 7, SOFT_PIECES[1], 0.0)
    rest = jnp.where(row == 6, SOFT_PIECES[2], 0.0)
    zero = jnp.zeros_like(x)
    h2, m2, l2 = -2.0 * h, -2.0 * m, -2.0 * l
    return jnp.concatenate([pair(h2, m2), pair(l2, h2), pair(m2, l2), pair(h2, m2), l2, ones,
                            ones, pair(a1, a2) + soft, pair(b1, b2) + rest, zero], axis=0)


def kernel(sizes, st_hbm, cell_hbm, w_hbm, m_hbm, data_hbm, model_ref, res_ref, search_ref,
           kmat, rhs, lhs, cell_v, w_v, m_all, st_all, szb, urow, acc, gacc, rb, rrow, qrow, grow,
           out1, out2, rs1, rs2, part1, part2, gather1, gather2, gmsg, gnmsg, gout, gnout, dout, din,
           in_sem, st_send, st_recv, m_sem, ar_send, ar_recv1, ar_recv2, ex_send, ex_recv1, ex_recv2,
           sc_send, sc_recv, data_v):
    n_sta, n_cell, cells, width, piece, scale = sizes
    nz = n_sta // 2
    chips = nz * n_cell
    tiles = 2 * cells // LANES
    half = cells // LANES
    groups = width // 8
    high = width // LANES
    per_tile = LANES // piece
    my_sta, my_cell = lax.axis_index("sta"), lax.axis_index("cell")
    core = lax.rem(my_sta, 2)
    z = lax.div(my_sta, 2)
    chip = z * n_cell + my_cell
    partner = (z * 2 + 1 - core, my_cell)

    def peer(k):
        flat = lax.rem(chip + k, chips)
        return (lax.div(flat, n_cell) * 2 + core, lax.rem(flat, n_cell))

    def every_peer(act):
        if chips > 16 or chips & (chips - 1) or n_cell & (n_cell - 1):
            def one(k, c):
                act(peer(k))
                return c

            lax.fori_loop(1, chips, one, 0)
        else:
            for k in range(chips - 1, 0, -1):
                act((my_sta ^ (k // n_cell * 2), my_cell ^ (k % n_cell)))

    def remote(src, dst, send, recv, device):
        return pltpu.make_async_remote_copy(src_ref=src, dst_ref=dst, send_sem=send, recv_sem=recv,
                                            device_id=device, device_id_type=MESH)

    def drain(ref, sem):
        pltpu.make_async_copy(ref, ref, sem).wait()

    barrier = pltpu.get_barrier_semaphore()

    around = [(lax.rem(z + k, nz) * 2 + core, my_cell) for k in range(1, nz)]
    around += [(my_sta, lax.rem(my_cell + k, n_cell)) for k in range(1, n_cell)]
    around.append(partner)
    for device in around:
        pl.semaphore_signal(barrier, inc=1, device_id=device, device_id_type=MESH)

    first_cell = pl.multiple_of(z * 2 * cells, 2 * cells)
    first_row = pl.multiple_of(z * tiles, tiles)
    load_cells = pltpu.make_async_copy(cell_hbm.at[:, pl.ds(first_cell, 2 * cells)], cell_v, in_sem.at[0])
    load_stations = pltpu.make_async_copy(st_hbm, st_all.at[z], in_sem.at[1])
    load_weights = pltpu.make_async_copy(w_hbm.at[pl.ds(first_row, tiles)], w_v, in_sem.at[2])
    load_model = pltpu.make_async_copy(m_hbm, m_all.at[core], in_sem.at[3])
    load_stations.start()
    load_cells.start()
    load_weights.start()
    load_model.start()
    load_data = pltpu.make_async_copy(data_hbm, data_v, in_sem.at[4])
    load_data.start()

    lot = min(2048, 2 * cells)

    def features(n, c):
        cols = pl.ds(pl.multiple_of(n * lot, lot), lot)
        rhs[:, cols] = cell_features(eight_rows(cell_v[:, cols]))
        return c

    def prepare(b):
        x = eight_rows(st_all[b])
        feats = station_features(x)
        for i in range(high):
            cols = slice(i * LANES, (i + 1) * LANES)
            lhs[cols, :] = jnp.transpose(feats[:, cols]).astype(BF16)
            zz = jnp.transpose(jnp.broadcast_to(x[2:3, cols], (LANES, LANES)))
            szb[i * 16:(i + 1) * 16] = zz.reshape(16, 8, LANES)

    block = min(2048, 2 * cells)

    def build(b, n):
        at = pl.multiple_of(n * block, block)
        r2 = jnp.dot(lhs[...], rhs[:, pl.ds(at, block)], preferred_element_type=F32)
        r2 = r2.reshape(groups, 8, block)
        cz = cell_v[2:3, pl.ds(at, block)]
        out = []
        for t in range(block // LANES):
            cols = slice(t * LANES, (t + 1) * LANES)
            inv = lax.rsqrt(r2[:, :, cols])
            dz = szb[...] - jnp.broadcast_to(cz[:, cols], (8, LANES))[None]
            out.append((dz * inv) * (inv * inv))
        kmat[pl.ds(b * groups, groups), :, pl.ds(at, block)] = jnp.concatenate(out, axis=2)

    def build_from(b, first):
        def one(n, c):
            build(b, n)
            return c

        lax.fori_loop(first, 2 * cells // block, one, 0)

    step = 8

    def forward(b, h, add):
        us = [jnp.broadcast_to(urow[pl.ds(h * half + t, 1), :], (8, LANES)) for t in range(half)]

        def some(i, c):
            for j in range(step):
                g = i * step + j
                sums = [None] * 4
                for t in range(half):
                    cols = pl.ds(pl.multiple_of(h * cells + t * LANES, LANES), LANES)
                    value = kmat[b * groups + g, :, cols] * us[t]
                    sums[t % 4] = value if sums[t % 4] is None else sums[t % 4] + value
                value = (sums[0] + sums[1]) + (sums[2] + sums[3])
                acc[b * groups + g] = value + acc[b * groups + g] if add else value
            return c

        lax.fori_loop(0, groups // step, some, 0)

    def block_rows(b):
        rows = []
        for i in range(high):
            x = acc[pl.ds(b * groups + i * 16, 16)].reshape(LANES, LANES)
            rows.append(jnp.sum(jnp.transpose(x), axis=0, keepdims=True))
        return jnp.concatenate(rows, axis=0)

    def keep_rows(rows, out, rs, b):
        out[b] = rows
        rs[b, chip] = rows

    def send_kept(out, rs, recv, b, which):
        every_peer(lambda device: remote(out.at[b], rs.at[b, chip], ar_send.at[which], recv.at[b],
                                         device).start())

    def send_rows(rows, out, rs, recv, b, which=0):
        keep_rows(rows, out, rs, b)
        send_kept(out, rs, recv, b, which)

    def broadcast(value, out, msgs, which):
        out[...] = value
        msgs[chip] = value

        every_peer(lambda device: remote(out, msgs.at[chip], sc_send.at[which], sc_recv.at[which],
                                         device).start())

    low = z < nz // 2

    def order(k):
        if nz < 2 or nz & (nz - 1):
            return lax.rem(z + k, nz)
        far = nz // 2
        return jnp.where(low & (k > 0) & (k <= far), far + k - 1, z ^ jnp.where(low & (k > far), k - far, k))

    def fixed(j):
        return nz - 1 - j

    def settled(j):
        far = nz // 2
        return jnp.where(j < far, jnp.where(j + far < nz, far + j, j),
                         jnp.where(low, nz - 1 - j, j - far))

    load_stations.wait()
    prepare(z)
    load_cells.wait()
    lax.fori_loop(0, 2 * cells // lot, features, 0)

    def enter():
        pl.semaphore_wait(barrier, len(around))

        def send_stations(k, c):
            other = lax.rem(z + k, nz)
            remote(st_all.at[z], st_all.at[z], st_send, st_recv.at[z], (other * 2 + core, my_cell)).start()
            return c

        lax.fori_loop(1, nz, send_stations, 0)
        remote(m_all.at[core], m_all.at[core], m_sem.at[0], m_sem.at[1], partner).start()

    load_model.wait()
    pl.when((z == nz - 1) & (z > 0))(enter)
    build(z, 0)
    pl.when((z > 0) & (z < nz - 1))(enter)
    build_from(z, 1)
    pl.when(z == 0)(enter)
    load_weights.wait()
    ws = w_v[...] * scale
    w_v[...] = ws
    drain(m_all.at[0], m_sem.at[1])
    urow[...] = ws * m_all[...].reshape(tiles, LANES)

    forward(z, 0, False)
    forward(z, 1, True)

    def stations_of(k):
        drain(st_all.at[order(k)], st_recv.at[order(k)])

    def own_rows():
        load_data.wait()
        lane = lax.broadcasted_iota(jnp.int32, (1, LANES), 1)
        wide = jnp.where(lane < piece, jnp.concatenate([data_v[...]] * per_tile, axis=1), 0.0)
        rows = [jnp.zeros((1, LANES), F32)] * high
        for q in range(n_cell):
            tile, at = q // per_tile, q % per_tile
            value = pltpu.roll(wide, at * piece, 1) if at else wide
            rows[tile] = jnp.where(my_cell == q, value, rows[tile])
        return block_rows(z) - jnp.concatenate(rows, axis=0)

    if nz > 1:
        stations_of(1)
        keep_rows(own_rows(), out1, rs1, z)
        prepare(order(1))
        build_from(order(1), 0)
        forward(order(1), 0, False)
        forward(order(1), 1, True)
    else:
        keep_rows(own_rows(), out1, rs1, z)

    def rest(k, c):
        b = order(k)

        @pl.when(k == 2)
        def _():
            for i in range(2, nz):
                stations_of(i)
            send_kept(out1, rs1, ar_recv1, z, 0)

        rows = block_rows(order(k - 1))
        prepare(b)
        send_rows(rows, out1, rs1, ar_recv1, order(k - 1))
        build_from(b, 0)
        forward(b, 0, False)
        forward(b, 1, True)
        return c

    lax.fori_loop(2, nz, rest, 0)
    if nz < 3:
        send_kept(out1, rs1, ar_recv1, z, 0)
    if nz > 1:
        send_rows(block_rows(order(nz - 1)), out1, rs1, ar_recv1, order(nz - 1))

    def arrive(b, rs, recv, store, sign):
        drain(rs.at[b, pl.ds(0, chips - 1)], recv.at[b])
        row = sign * jnp.sum(rs[b], axis=0)
        store[b] = row
        for i in range(high):
            x = jnp.transpose(jnp.broadcast_to(row[i:i + 1], (LANES, LANES)))
            rb[i * 16:(i + 1) * 16] = x.reshape(16, 8, LANES)

    strip = 16

    def backward(b, at):
        x = kmat[pl.ds(b * groups, groups), :, pl.ds(pl.multiple_of(at * LANES, LANES), strip * LANES)]
        return [gacc[at + t] + jnp.sum(x[:, :, t * LANES:(t + 1) * LANES] * rb[...], axis=0)
                for t in range(strip)]

    def gradient(turn, rs, recv, store, sign, part, gather, send, ex_recv, complete):
        gacc[...] = jnp.zeros((tiles, 8, LANES), F32)

        def early(j, c):
            b = turn(j)
            arrive(b, rs, recv, store, sign)

            def some(i, c):
                for t, total in enumerate(backward(b, i * strip)):
                    gacc[i * strip + t] = total
                return c

            lax.fori_loop(0, tiles // strip, some, 0)
            return c

        lax.fori_loop(0, nz - 1, early, 0)
        b = turn(nz - 1)
        arrive(b, rs, recv, store, sign)
        complete()
        for h in range(2):
            def some(i, c):
                rows = [jnp.sum(a, axis=0, keepdims=True) for a in backward(b, h * half + i * strip)]
                part[h, pl.ds(pl.multiple_of(i * strip, strip), strip)] = jnp.concatenate(rows, axis=0)
                return c

            lax.fori_loop(0, half // strip, some, 0)
            remote(part.at[h], gather.at[h], send, ex_recv.at[h], partner).start()

    gradient(settled, rs1, ar_recv1, rrow, -1.0, part1, gather1, ex_send.at[0], ex_recv1, lambda: None)
    for h in range(2):
        drain(gather1.at[h], ex_recv1.at[h])
        rows = slice(h * half, (h + 1) * half)
        g = w_v[rows] * (part1[h] + gather1[h])
        grow[rows] = g
        urow[rows] = w_v[rows] * g
        if h == 0:
            forward(fixed(0), 0, False)
    def image(j, c):
        b = fixed(j)

        @pl.when(j >= 1)
        def _():
            forward(b, 0, False)

        forward(b, 1, True)
        send_rows(block_rows(b), out2, rs2, ar_recv2, b, 1)
        return c

    lax.fori_loop(0, nz, image, 0)
    g = grow[...]
    broadcast(jnp.sum(g * g, axis=0, keepdims=True), gout, gmsg, 0)

    def send_delta():
        q = qrow[...]
        dout[...] = jnp.sum(jnp.sum(q * q, axis=0), axis=0, keepdims=True)
        remote(dout, din, sc_send.at[1], sc_recv.at[1], partner).start()

    gradient(fixed, rs2, ar_recv2, qrow, 1.0, part2, gather2, ex_send.at[1], ex_recv2, send_delta)

    def total(msgs, which):
        drain(msgs.at[pl.ds(0, chips - 1)], sc_recv.at[which])
        return jnp.sum(jnp.sum(msgs[...], axis=0), axis=1, keepdims=True)

    gamma = total(gmsg, 0)
    drain(din, sc_recv.at[1])
    alpha = gamma / jnp.sum(dout[...] + din[...], axis=1, keepdims=True)

    own = pl.ds(pl.multiple_of(core * half, half), half)
    model_ref[...] = m_all[core] + alpha * grow[own]
    new = rrow[z] - alpha * qrow[z]
    mine = jnp.zeros((1, LANES), F32)
    for q in range(n_cell):
        tile, at = q // per_tile, q % per_tile
        value = new[tile:tile + 1]
        if at:
            value = pltpu.roll(value, LANES - at * piece, 1)
        mine = jnp.where(my_cell == q, value, mine)
    res_ref[...] = mine[:, :piece]

    square = jnp.zeros((half, LANES), F32)
    for h in range(2):
        drain(gather2.at[h], ex_recv2.at[h])
        rows = slice(h * half, (h + 1) * half)
        g = grow[rows] - alpha * (w_v[rows] * (part2[h] + gather2[h]))
        urow[rows] = g
        square += g * g
    value = jnp.sum(square, axis=0, keepdims=True)
    gnout[...] = value
    gnmsg[chip] = value

    def tell(device):
        for sta in (device[0] ^ 1, device[0]):
            remote(gnout, gnmsg.at[chip], sc_send.at[2], sc_recv.at[2], (sta, device[1])).start()

    pl.when(core == 1)(lambda: every_peer(tell))
    drain(st_all.at[pl.ds(0, nz - 1)], st_send)
    drain(m_all.at[0], m_sem.at[0])
    drain(rs1.at[:, pl.ds(0, chips - 1)], ar_send.at[0])
    drain(rs2.at[:, pl.ds(0, chips - 1)], ar_send.at[1])
    drain(part1, ex_send.at[0])
    drain(part2, ex_send.at[1])
    drain(gmsg.at[pl.ds(0, chips - 1)], sc_send.at[0])
    drain(din, sc_send.at[1])
    beta = total(gnmsg, 2) / gamma
    search_ref[...] = urow[own] + beta * grow[own]

    @pl.when(core == 1)
    def _():
        for _ in range(2):
            drain(gnmsg.at[pl.ds(0, chips - 1)], sc_send.at[2])


def per_device(station_xyz, cell_xyz, cell_weight, data, model_start):
    n_sta, n_cell = lax.axis_size("sta"), lax.axis_size("cell")
    n = n_sta * n_cell
    width = station_xyz.shape[1]
    cells = model_start.shape[0]
    piece = data.shape[0]
    scale = 1.0 / math.sqrt(width * n_sta * cells * n)
    sizes = (n_sta, n_cell, cells, width, piece, scale)
    nz = n_sta // 2
    chips = nz * n_cell
    tiles, half = 2 * cells // LANES, cells // LANES
    groups, high = width // 8, width // LANES
    hbm = pl.BlockSpec(memory_space=pltpu.HBM)
    vmem = pl.BlockSpec(memory_space=pltpu.VMEM)
    spread = pltpu.VMEM((nz * groups, 8, LANES), F32)
    narrow = pltpu.VMEM((groups, 8, LANES), F32)
    lines = pltpu.VMEM((nz, high, LANES), F32)
    whole = pltpu.VMEM((nz, chips, high, LANES), F32)
    halves = pltpu.VMEM((2, half, LANES), F32)
    packed = pltpu.VMEM((tiles, LANES), F32)
    message = pltpu.VMEM((chips, 1, LANES), F32)
    row = pltpu.VMEM((1, LANES), F32)
    dma = pltpu.SemaphoreType.DMA
    model_next, residual, search = pl.pallas_call(
        functools.partial(kernel, sizes),
        out_shape=(jax.ShapeDtypeStruct((half, LANES), F32), jax.ShapeDtypeStruct((1, piece), F32),
                   jax.ShapeDtypeStruct((half, LANES), F32)),
        in_specs=[hbm] * 5,
        out_specs=(vmem, vmem, vmem),
        scratch_shapes=[
            pltpu.VMEM((nz * groups, 8, 2 * cells), F32),
            pltpu.VMEM((FEATURES, 2 * cells), BF16),
            pltpu.VMEM((width, FEATURES), BF16),
            pltpu.VMEM((3, 2 * cells), F32),
            packed, halves,
            pltpu.VMEM((nz, 3, width), F32),
            narrow, packed, spread,
            pltpu.VMEM((tiles, 8, LANES), F32),
            narrow, lines, lines, packed,
            lines, lines, whole, whole,
            halves, halves, halves, halves,
            message, message, row, row, row, row,
            dma((5,)), dma, dma((nz,)), dma((2,)), dma((2,)), dma((nz,)), dma((nz,)),
            dma((2,)), dma((2,)), dma((2,)), dma((3,)), dma((3,)),
            pltpu.VMEM((1, piece), F32),
        ],
        compiler_params=pltpu.CompilerParams(
            collective_id=0, has_side_effects=True, vmem_limit_bytes=48 * 1024 * 1024),
    )(*[pltpu.with_memory_space_constraint(x, pltpu.HBM) for x in (station_xyz, cell_xyz, cell_weight.reshape(-1, LANES), model_start.reshape(-1, LANES),
      data.reshape(1, piece))])
    def hand(a, b, c, x, y, z):
        x[...] = a[...]
        y[...] = b[...]
        z[...] = c[...]

    model_next, residual, search = pl.pallas_call(
        hand,
        out_shape=(jax.ShapeDtypeStruct((half, LANES), F32), jax.ShapeDtypeStruct((1, piece), F32),
                   jax.ShapeDtypeStruct((half, LANES), F32)),
        in_specs=[vmem] * 3, out_specs=(vmem, vmem, vmem),
        compiler_params=pltpu.CompilerParams(vmem_limit_bytes=1024 * 1024),
    )(model_next, residual, search)
    return (model_next.reshape(cells), residual.reshape(piece), search.reshape(cells))


def solution(mesh):
    placed = (P(None, "sta"), P(None, "cell"), P("cell"), P(("sta", "cell")), P(("cell", "sta")))
    return jax.shard_map(
        per_device,
        mesh=mesh,
        in_specs=placed,
        out_specs=(P(("cell", "sta")), P(("sta", "cell")), P(("cell", "sta"))),
        check_vma=False,
    )
```
